512 devices in a mesh: utt: 8 (over y, z_hi), tm: 64 (over x, z_lo, core).
Axes of the slice: x: 4, y: 4, z: 16 (z_hi: 2, z_lo: 8; z = z_hi * 8 + z_lo), core: 2. Of those that a mesh axis runs over, the one named last changes fastest.
Arguments:
- stem: bfloat16 [65536, 1280], P(('utt', 'tm')), parts along dimension 0, may hold values from -8 to 8
- norm_gain: float32 [1280], replicated, may hold values from 0.25 to 1.75
- qkv_weight: bfloat16 [1280, 3840], P('tm'), may hold values from -0.2934839 to 0.2934839
- segment_ids: int32 [65536], P(('utt', 'tm')), parts along dimension 0, may hold values from 1 to 21, as said below
- dec_queries: bfloat16 [1024, 1280], P(('utt', 'tm')), parts along dimension 0, may hold values from -9 to 9
- stretch_mask: int32 [1024, 64], P(('utt', 'tm')), parts along dimension 0, may hold values 0 or 1
Outputs:
- memory: bfloat16 [65536, 1280], P(('utt', 'tm')), parts along dimension 0
- cross_out: bfloat16 [1024, 1280], P(('utt', 'tm')), parts along dimension 0
The draws below stay inside these ranges and needn't reach their ends.
There are 8 independent parts, one for each index of `utt`. The reference program is written for one: setup_inputs(seed, part) draws one part's arguments, and reference() takes and returns one part's arrays. A program takes and returns all parts, laid end to end along the dimension named above; an argument that names none is the same for every part. Nothing has to cross between parts.
Inputs may be any that keep to these rules, and one draw needn't show every extreme that they name: `segment_ids`: ids start at 1 and rise by one from run to run; each id covers one contiguous run of at most 512 positions, and the last run is exactly 512 positions long.
All inputs are finite; a program needn't handle non-finite values. No bound on the sum of `stretch_mask` on one device may be relied on, other than what follows from the above.
Results may differ from the reference program's by a relative error of at most 0.0062.
Values may be sent and summed in bfloat16 or wider, within the bound.
A program may use at most 64 MiB of HBM per device.

```python
import jax
import jax.numpy as jnp
from jax import lax

H = 20
HD = 64
D = 1280
POS_DEV = 128
DTOK_DEV = 2
WINDOW = 512
POS = 8192
DTOK = 128
STRETCHES = 64
N_TM = 64


def loud_pattern(key):
    flips = jax.random.bernoulli(jax.random.fold_in(key, 7), 0.5, (D,))
    return jnp.where(flips, 1.0, -1.0).astype(jnp.float32)


def loud_rows(key, count, share, lowest):
    pattern = loud_pattern(key)
    noise_key, pick_key, level_key = jax.random.split(key, 3)
    noise = jnp.clip(jax.random.normal(noise_key, (count, D), jnp.float32), -4.0, 4.0)
    loud = jax.random.bernoulli(pick_key, share, (count, 1))
    amplitude = lowest + 1.5 * jax.random.randint(level_key, (count, 1), 0, 3).astype(jnp.float32)
    return jnp.where(loud, amplitude * pattern[None, :] + 0.6 * noise, noise)


def draw_stem(key, part):
    return loud_rows(jax.random.fold_in(key, 11), POS, 1.0 / 32.0, 2.5).astype(jnp.bfloat16)


def draw_dec_queries(key, part):
    return loud_rows(jax.random.fold_in(key, 13), DTOK, 1.0 / 8.0, 3.0).astype(jnp.bfloat16)


def draw_qkv_weight(key, part):
    base_key = jax.random.fold_in(key, 0)
    whole = jnp.clip(jax.random.normal(base_key, (D, 3 * D), jnp.float32), -4.0, 4.0) * D ** (-0.5)
    return whole.astype(jnp.bfloat16)


def draw_segment_ids(key, part):
    runs = (N_TM - 4) // 3
    margin = POS_DEV // 4
    shifts = jax.random.randint(key, (runs - 1,), -margin, margin + 1, dtype=jnp.int32)
    marks = jnp.arange(1, runs, dtype=jnp.int32)
    inner = marks * ((N_TM - 4) * POS_DEV) // runs + shifts
    cuts = jnp.concatenate([inner, jnp.full((1,), POS - 4 * POS_DEV, jnp.int32)])
    places = jnp.arange(POS, dtype=jnp.int32)
    passed = jnp.sum((places[:, None] >= cuts[None, :]).astype(jnp.int32), axis=1)
    return (passed + 1).astype(jnp.int32)


def place_ends(values, own_key, least, top_value):
    shape = values.shape
    index_at = [jax.random.randint(jax.random.fold_in(own_key, axis), (), 0, shape[axis]) for axis in range(len(shape))]
    values = values.at[tuple(index_at)].set(least)
    longest = shape.index(max(shape))
    index_at[longest] = (index_at[longest] + 1) % shape[longest]
    return values.at[tuple(index_at)].set(top_value)


def setup_inputs(seed: int = 0, part: int = 0) -> dict:
    streams_of = jax.random.split(jax.random.key(seed), 7)
    own_keys = jax.random.split(jax.random.fold_in(streams_of[6], part), 7)
    return {
        "stem": draw_stem(jax.random.fold_in(jax.random.fold_in(streams_of[6], part), 71), part),
        "norm_gain": jnp.clip(1.0 + 0.15 * jax.random.normal(streams_of[1], (D,), jnp.float32), 0.25, 1.75),
        "qkv_weight": draw_qkv_weight(jax.random.fold_in(streams_of[6], 71), part),
        "segment_ids": draw_segment_ids(jax.random.fold_in(jax.random.fold_in(streams_of[6], part), 71), part),
        "dec_queries": draw_dec_queries(jax.random.fold_in(jax.random.fold_in(streams_of[6], part), 71), part),
        "stretch_mask": place_ends((jax.random.randint(own_keys[5], (DTOK, STRETCHES), 0, 2) < 1).astype(jnp.int32), jax.random.fold_in(own_keys[5], 1), 0, 1),
    }


def layer_norm(stem, norm_gain):
    values = stem.astype(jnp.float32)
    mean = lax.optimization_barrier(jnp.mean(values, axis=-1, keepdims=True))
    var = lax.optimization_barrier(jnp.mean((values - mean) ** 2, axis=-1, keepdims=True))
    return ((values - mean) * lax.rsqrt(var + 1e-05) * norm_gain).astype(jnp.bfloat16)

def reference(stem, norm_gain, qkv_weight, segment_ids, dec_queries, stretch_mask):
    scale = HD ** (-0.5)
    normed = layer_norm(stem, norm_gain)
    projected = jnp.dot(normed, qkv_weight, preferred_element_type=jnp.float32).astype(jnp.bfloat16)
    queries = projected[:, :D]
    keyvals = projected[:, D:]
    zero_rows = jnp.zeros((WINDOW, 2 * D), jnp.bfloat16)
    padded = jnp.concatenate([zero_rows, keyvals, zero_rows], axis=0)
    zero_ids = jnp.full((WINDOW,), -1, jnp.int32)
    seg_padded = jnp.concatenate([zero_ids, segment_ids.astype(jnp.int32), zero_ids], axis=0)
    extent = 2 * WINDOW + POS_DEV

    def block(index):
        start = (index * POS_DEV).astype(jnp.int32)
        qblock = lax.dynamic_slice_in_dim(queries, start, POS_DEV, 0).reshape(POS_DEV, H, HD).astype(jnp.float32)
        kvblock = lax.dynamic_slice_in_dim(padded, start, extent, 0)
        keys = kvblock[:, :D].reshape(extent, H, HD).astype(jnp.float32)
        values = kvblock[:, D:].reshape(extent, H, HD).astype(jnp.float32)
        seg_q = lax.dynamic_slice_in_dim(segment_ids.astype(jnp.int32), start, POS_DEV, 0)
        seg_k = lax.dynamic_slice_in_dim(seg_padded, start, extent, 0)
        scores = jnp.einsum('qhd,khd->hqk', qblock, keys) * scale
        same = seg_q[:, None] == seg_k[None, :]
        scores = jnp.where(same[None], scores, jnp.float32(-1e+30))
        top = lax.optimization_barrier(jnp.max(scores, axis=-1, keepdims=True))
        raised = jnp.exp(scores - top)
        probs = (raised / lax.optimization_barrier(jnp.sum(raised, axis=-1, keepdims=True))).astype(jnp.bfloat16)
        context = jnp.einsum('hqk,khd->qhd', probs.astype(jnp.float32), values)
        return context.reshape(POS_DEV, D)
    contexts = lax.map(block, jnp.arange(N_TM, dtype=jnp.int32)).reshape(POS, D)
    memory = (stem.astype(jnp.float32) + contexts).astype(jnp.bfloat16)
    owner = jnp.arange(DTOK, dtype=jnp.int32) // DTOK_DEV
    stretch_index = jnp.arange(N_TM, dtype=jnp.int32)
    allowed = (stretch_mask == 1) | (owner[:, None] == stretch_index[None, :])
    head_queries = jnp.transpose(dec_queries.reshape(DTOK, H, HD), (1, 0, 2))
    head_memory = jnp.transpose(memory.reshape(POS, H, HD), (1, 0, 2))

    def one_head(pair):
        query, mem = pair
        cross = jnp.dot(query, mem.T, preferred_element_type=jnp.float32) * scale
        cross = cross.reshape(DTOK, N_TM, POS_DEV)
        top = lax.optimization_barrier(jnp.max(cross, axis=-1))
        raised = jnp.where(allowed[:, :, None], jnp.exp(cross - top[:, :, None]), jnp.float32(0.0))
        den = lax.optimization_barrier(jnp.sum(raised, axis=-1))
        num = jnp.einsum('tcp,cpd->tcd', raised.astype(jnp.bfloat16).astype(jnp.float32), mem.reshape(N_TM, POS_DEV, HD).astype(jnp.float32))
        top_masked = jnp.where(allowed, top, jnp.float32(-1e+30))
        best = lax.optimization_barrier(jnp.max(top_masked, axis=1))
        factor = jnp.exp(top_masked - best[:, None])
        total = lax.optimization_barrier(jnp.sum(factor[:, :, None] * num, axis=1))
        return total / lax.optimization_barrier(jnp.sum(factor * den, axis=1))[:, None]
    heads_out = lax.map(one_head, (head_queries, head_memory))
    cross_out = jnp.transpose(heads_out, (1, 0, 2)).reshape(DTOK, D).astype(jnp.bfloat16)
    return (memory, cross_out)
```

```python
import math

import jax
import jax.numpy as jnp
from jax import lax
from jax.sharding import PartitionSpec as P

HD = 64


def from_behind(block, axis, distance):
    devices = range(lax.axis_size(axis))
    route = [(i - distance, i) for i in devices if i - distance in devices]
    return lax.ppermute(block, axis, route)


def on_device(stem, norm_gain, qkv_weight, segment_ids, dec_queries, stretch_mask):
    rows, width = stem.shape
    heads = width // HD
    scale = HD ** (-0.5)
    tokens_dev = dec_queries.shape[0]
    n_tm = lax.axis_size("tm")
    device = lax.axis_index("tm")
    small = jnp.concatenate(
        [
            dec_queries.reshape(-1),
            stretch_mask.astype(jnp.bfloat16).reshape(-1),
            (segment_ids % 128).astype(jnp.bfloat16),
            (segment_ids // 128).astype(jnp.bfloat16),
        ]
    )
    cuts = [tokens_dev * width, tokens_dev * (width + n_tm)]
    cuts += [cuts[1] + rows, cuts[1] + 2 * rows]
    depth, columns = qkv_weight.shape
    small = jnp.pad(small, (0, -cuts[3] % columns)).reshape(-1, columns)
    gathered = lax.all_gather(jnp.concatenate([qkv_weight, small], axis=0), "tm", axis=0)
    weight = gathered[:, :depth].reshape(n_tm * depth, columns)
    small_all = gathered[:, depth:].reshape(n_tm, -1)
    all_queries = small_all[:, : cuts[0]].reshape(n_tm * tokens_dev, width)
    all_masks = small_all[:, cuts[0] : cuts[1]].reshape(n_tm * tokens_dev, n_tm)
    seg_low = small_all[:, cuts[1] : cuts[2]].reshape(-1).astype(jnp.int32)
    seg_high = small_all[:, cuts[2] : cuts[3]].reshape(-1).astype(jnp.int32)
    seg_all = jnp.pad(seg_high * 128 + seg_low, (4 * rows, 4 * rows))
    seg_wide = lax.dynamic_slice_in_dim(seg_all, device * rows, 9 * rows, 0)
    values_in = stem.astype(jnp.float32)
    mean = jnp.mean(values_in, axis=-1, keepdims=True)
    var = jnp.mean((values_in - mean) ** 2, axis=-1, keepdims=True)
    normed = ((values_in - mean) * lax.rsqrt(var + 1e-05) * norm_gain).astype(jnp.bfloat16)
    projected = jnp.dot(
        normed,
        weight,
        preferred_element_type=jnp.float32,
    ).astype(jnp.bfloat16)
    query_part = projected[:, :width]
    keyvals = projected[:, width:]
    kv_pieces = []
    for offset in range(-4, 5):
        if offset == 0:
            kv_pieces.append(keyvals)
        else:
            kv_pieces.append(from_behind(keyvals, "tm", -offset))
    extended = jnp.concatenate(kv_pieces, axis=0)
    same = segment_ids[:, None] == seg_wide[None, :]
    group = math.gcd(heads, 4)
    span = group * HD
    groups = heads // group

    def attend(index):
        start = index * span
        query_group = lax.dynamic_slice_in_dim(query_part, start, span, 1).reshape(rows, group, HD)
        key_group = lax.dynamic_slice_in_dim(extended, start, span, 1).reshape(-1, group, HD)
        value_group = lax.dynamic_slice_in_dim(extended, width + start, span, 1).reshape(
            -1, group, HD
        )
        scores = (
            jnp.einsum("qhd,khd->hqk", query_group, key_group, preferred_element_type=jnp.float32)
            * scale
        )
        scores = jnp.where(same[None], scores, jnp.float32(-1e30))
        top = jnp.max(scores, axis=-1, keepdims=True)
        raised = jnp.exp(scores - top)
        probs = (raised / jnp.sum(raised, axis=-1, keepdims=True)).astype(jnp.bfloat16)
        context = jnp.einsum("hqk,khd->qhd", probs, value_group, preferred_element_type=jnp.float32)
        return context.reshape(rows, span)

    contexts = lax.map(attend, jnp.arange(groups, dtype=jnp.int32))
    context = jnp.transpose(contexts, (1, 0, 2)).reshape(rows, width)
    memory = (values_in + context).astype(jnp.bfloat16)
    total_tokens = all_queries.shape[0]
    column = lax.dynamic_slice_in_dim(all_masks, device, 1, 1)[:, 0]
    owner = jnp.arange(total_tokens, dtype=jnp.int32) // tokens_dev
    allowed = (column == 1) | (owner == device)
    query_heads = all_queries.reshape(total_tokens, heads, HD)
    memory_heads = memory.reshape(rows, heads, HD)
    cross = (
        jnp.einsum("thd,phd->htp", query_heads, memory_heads, preferred_element_type=jnp.float32)
        * scale
    )
    local_top = jnp.max(cross, axis=-1)
    weights = jnp.where(
        allowed[None, :, None], jnp.exp(cross - local_top[:, :, None]), jnp.float32(0.0)
    )
    denom = jnp.transpose(jnp.sum(weights, axis=-1))
    numer = jnp.einsum(
        "htp,phd->thd",
        weights.astype(jnp.bfloat16),
        memory_heads,
        preferred_element_type=jnp.float32,
    )
    top_masked = jnp.transpose(jnp.where(allowed[None, :], local_top, jnp.float32(-1e30)))
    packed = jnp.concatenate([numer.reshape(total_tokens, width), top_masked, denom], axis=1)
    packed = jnp.pad(packed, ((0, 0), (0, -packed.shape[1] % 128)))
    packed = packed.reshape(n_tm, tokens_dev, -1)
    got = lax.all_to_all(packed, "tm", split_axis=0, concat_axis=0, tiled=True)
    num_all = got[..., :width].reshape(n_tm, tokens_dev, heads, HD)
    top_all = got[..., width : width + heads]
    den_all = got[..., width + heads : width + 2 * heads]
    best = jnp.max(top_all, axis=0)
    factor = jnp.exp(top_all - best[None])
    num_total = jnp.sum(factor[..., None] * num_all, axis=0)
    den_total = jnp.sum(factor * den_all, axis=0)
    cross_out = (num_total / den_total[..., None]).reshape(tokens_dev, width).astype(jnp.bfloat16)
    return (memory, cross_out)


def solution(mesh):
    placed = (
        P(("utt", "tm"), None),
        P(),
        P("tm", None),
        P(("utt", "tm")),
        P(("utt", "tm"), None),
        P(("utt", "tm"), None),
    )
    return jax.shard_map(
        on_device,
        mesh=mesh,
        in_specs=placed,
        out_specs=(P(("utt", "tm"), None), P(("utt", "tm"), None)),
        check_vma=False,
    )
```

```python
import functools
import math

import jax
import jax.numpy as jnp
from jax import lax
from jax.experimental import pallas as pl
from jax.experimental.pallas import tpu as pltpu
from jax.sharding import PartitionSpec as P

HD = 64
NZ = 8
REACH = 2
MESH = pl.DeviceIdType.MESH


def gather_kernel(nx, w_ref, stem_ref, wide_ref, halo_ref, w_recv, w_zs, w_xs, w_ps, h_recv, h_zs, h_ps, own_sem):
    me = lax.axis_index("tm")
    core = lax.rem(me, 2)
    chip = me // 2
    z = lax.rem(chip, NZ)
    x = chip // NZ
    chips = nx * NZ

    def index(xx, zz):
        return (xx * NZ + zz) * 2 + core

    right_x, left_x, far_x = lax.rem(x + 1, nx), lax.rem(x + nx - 1, nx), lax.rem(x + 2, nx)
    right, left = index(right_x, z), index(left_x, z)
    partner = me + 1 - 2 * core
    up, down = me + 2, me - 2
    has_up, has_down = z < NZ - 1, z > 0
    has_next, has_prev = chip < chips - 1, chip > 0

    barrier = pltpu.get_barrier_semaphore()

    def greet(peer):
        pl.semaphore_signal(barrier, inc=1, device_id={"tm": peer}, device_id_type=MESH)

    greet(right)
    greet(left)
    greet(partner)

    @pl.when(has_next)
    def _():
        greet(up)

    @pl.when(has_prev)
    def _():
        greet(down)

    pl.semaphore_wait(barrier, 3 + has_next.astype(jnp.int32) + has_prev.astype(jnp.int32))

    def w_copy(shard, peer, send_sem, own=False):
        return pltpu.make_async_remote_copy(
            src_ref=w_ref if own else wide_ref.at[shard],
            dst_ref=wide_ref.at[shard],
            send_sem=send_sem,
            recv_sem=w_recv.at[shard],
            device_id={"tm": peer},
            device_id_type=MESH,
        )

    def h_copy(from_slot, to_slot, peer, send_sem, own=False):
        return pltpu.make_async_remote_copy(
            src_ref=stem_ref if own else halo_ref.at[from_slot],
            dst_ref=halo_ref.at[to_slot],
            send_sem=send_sem,
            recv_sem=h_recv.at[to_slot],
            device_id={"tm": peer},
            device_id_type=MESH,
        )

    def to_right(xx, zz, slot, own=False):
        return w_copy(index(xx, zz), right, w_xs.at[0, slot * NZ + zz], own)

    def to_left(xx, zz, slot, own=False):
        return w_copy(index(xx, zz), left, w_xs.at[1, slot * NZ + zz], own)

    def to_partner(xx, zz, own=False):
        return w_copy(index(xx, zz), partner, w_ps.at[xx * NZ + zz], own)

    def to_up(zz, own=False):
        return w_copy(index(x, zz), up, w_zs.at[0, zz], own)

    def to_down(zz, own=False):
        return w_copy(index(x, zz), down, w_zs.at[1, zz], own)

    def slot_of(step, cc):
        return (step + REACH) * 2 + cc

    own_slot = slot_of(0, core)
    h_next = h_copy(own_slot, slot_of(-1, core), up, h_zs.at[0], True)
    h_prev = h_copy(own_slot, slot_of(1, core), down, h_zs.at[1], True)
    h_own = h_copy(own_slot, own_slot, partner, h_ps.at[2], True)
    relay_next = h_copy(slot_of(-1, core), slot_of(-2, core), up, h_zs.at[2])
    relay_prev = h_copy(slot_of(1, core), slot_of(2, core), down, h_zs.at[3])

    def h_pass(step):
        slot = slot_of(step, core)
        return h_copy(slot, slot, partner, h_ps.at[step + REACH])

    def w_arrived(shard):
        pltpu.make_async_copy(wide_ref.at[shard], wide_ref.at[shard], w_recv.at[shard]).wait()

    def h_arrived(slot):
        pltpu.make_async_copy(halo_ref.at[slot], halo_ref.at[slot], h_recv.at[slot]).wait()

    @pl.when(has_up)
    def _():
        to_up(z, True).start()

    @pl.when(has_down)
    def _():
        to_down(z, True).start()

    @pl.when(has_next)
    def _():
        h_next.start()

    @pl.when(has_prev)
    def _():
        h_prev.start()

    to_right(x, z, 0, True).start()
    to_left(x, z, 0, True).start()
    to_partner(x, z, True).start()
    h_own.start()
    own_w = pltpu.make_async_copy(w_ref, wide_ref.at[me], own_sem.at[0])
    own_h = pltpu.make_async_copy(stem_ref, halo_ref.at[own_slot], own_sem.at[1])
    own_w.start()
    own_h.start()

    def beside(zz, fresh):
        ok = (zz >= 0) & (zz < NZ) & fresh

        @pl.when(ok)
        def _():
            even = lax.rem(zz, 2) == 0
            w_arrived(index(left_x, zz))
            to_partner(left_x, zz).start()

            @pl.when(even)
            def _():
                to_right(left_x, zz, 1).start()

            w_arrived(index(right_x, zz))
            to_partner(right_x, zz).start()

            @pl.when(jnp.logical_not(even))
            def _():
                to_left(right_x, zz, 1).start()

    def far(zz, fresh):
        @pl.when((zz >= 0) & (zz < NZ) & fresh)
        def _():
            w_arrived(index(far_x, zz))
            to_partner(far_x, zz).start()

    def step(s, carry):
        below, above = z - s, z + s

        @pl.when((below >= 0) & (s > 0) & (s < NZ))
        def _():
            w_arrived(index(x, below))

            @pl.when(has_up)
            def _():
                to_up(below).start()

            to_right(x, below, 0).start()
            to_left(x, below, 0).start()
            to_partner(x, below).start()

        @pl.when((above < NZ) & (s > 0))
        def _():
            w_arrived(index(x, above))

            @pl.when(has_down)
            def _():
                to_down(above).start()

            to_right(x, above, 0).start()
            to_left(x, above, 0).start()
            to_partner(x, above).start()

        beside(z - (s - 1), s >= 1)
        beside(z + (s - 1), s >= 2)
        far(z - (s - 2), s >= 2)
        far(z + (s - 2), s >= 3)
        return carry

    lax.fori_loop(1, 4, step, 0)

    @pl.when(has_prev)
    def _():
        h_arrived(slot_of(-1, core))
        h_pass(-1).start()

        @pl.when(has_next)
        def _():
            relay_next.start()

    @pl.when(has_next)
    def _():
        h_arrived(slot_of(1, core))
        h_pass(1).start()

        @pl.when(has_prev)
        def _():
            relay_prev.start()

    lax.fori_loop(4, NZ + 2, step, 0)

    @pl.when(chip >= 2)
    def _():
        h_arrived(slot_of(-2, core))
        h_pass(-2).start()

    @pl.when(chip < chips - 2)
    def _():
        h_arrived(slot_of(2, core))
        h_pass(2).start()

    def settle(i, carry):
        w_arrived(i * 2 + 1 - core)
        to_partner(i // NZ, lax.rem(i, NZ), False).wait_send()
        return carry

    lax.fori_loop(0, chips, settle, 0)

    def settle_z(zz, carry):
        @pl.when((zz <= z) & has_up)
        def _():
            to_up(zz).wait_send()

        @pl.when((zz >= z) & has_down)
        def _():
            to_down(zz).wait_send()

        to_right(x, zz, 0).wait_send()
        to_left(x, zz, 0).wait_send()
        even = lax.rem(zz, 2) == 0

        @pl.when(even)
        def _():
            to_right(left_x, zz, 1).wait_send()

        @pl.when(jnp.logical_not(even))
        def _():
            to_left(right_x, zz, 1).wait_send()

        return carry

    lax.fori_loop(0, NZ, settle_z, 0)

    def other(step):
        h_arrived(slot_of(step, 1 - core))

    other(0)
    h_own.wait_send()

    @pl.when(has_next)
    def _():
        h_next.wait_send()
        h_pass(1).wait_send()
        other(1)

    @pl.when(has_prev)
    def _():
        h_prev.wait_send()
        h_pass(-1).wait_send()
        other(-1)

    @pl.when(has_next & has_prev)
    def _():
        relay_next.wait_send()
        relay_prev.wait_send()

    @pl.when(chip >= 2)
    def _():
        h_pass(-2).wait_send()
        other(-2)

    @pl.when(chip < chips - 2)
    def _():
        h_pass(2).wait_send()
        other(2)

    own_w.wait()
    own_h.wait()


def gather(wide, stem, n_tm):
    nx = n_tm // (2 * NZ)
    dma = pltpu.SemaphoreType.DMA
    return pl.pallas_call(
        functools.partial(gather_kernel, nx),
        out_shape=(
            jax.ShapeDtypeStruct((n_tm, *wide.shape), wide.dtype),
            jax.ShapeDtypeStruct((4 * REACH + 2, *stem.shape), stem.dtype),
        ),
        in_specs=[pl.BlockSpec(memory_space=pltpu.VMEM)] * 2,
        out_specs=(pl.BlockSpec(memory_space=pl.ANY), pl.BlockSpec(memory_space=pl.ANY)),
        scratch_shapes=[
            dma((n_tm,)),
            dma((2, NZ)),
            dma((2, 2 * NZ)),
            dma((n_tm // 2,)),
            dma((4 * REACH + 2,)),
            dma((4,)),
            dma((2 * REACH + 1,)),
            dma((2,)),
        ],
        compiler_params=pltpu.CompilerParams(collective_id=0, has_side_effects=True),
        name="gather",
    )(wide, stem)


def deal_kernel(n, out_ref, in_ref, send_sem, recv_sem, own_sem):
    me = lax.axis_index("tm")
    barrier = pltpu.get_barrier_semaphore()

    def peer_of(i):
        return lax.rem(me + i, n)

    def greet(i, carry):
        pl.semaphore_signal(barrier, inc=1, device_id={"tm": peer_of(i)}, device_id_type=MESH)
        return carry

    lax.fori_loop(1, n, greet, 0)
    own = pltpu.make_async_copy(out_ref.at[me], in_ref.at[me], own_sem)
    own.start()
    pl.semaphore_wait(barrier, n - 1)

    def copy(i):
        peer = peer_of(i)
        return pltpu.make_async_remote_copy(
            src_ref=out_ref.at[peer],
            dst_ref=in_ref.at[me],
            send_sem=send_sem.at[i],
            recv_sem=recv_sem.at[me],
            device_id={"tm": peer},
            device_id_type=MESH,
        )

    def send(i, carry):
        copy(i).start()
        return carry

    lax.fori_loop(1, n, send, 0)
    own.wait()

    def settle(i, carry):
        peer = peer_of(i)
        pltpu.make_async_copy(in_ref.at[peer], in_ref.at[peer], recv_sem.at[peer]).wait()
        copy(i).wait_send()
        return carry

    lax.fori_loop(1, n, settle, 0)


def deal(payload):
    n = payload.shape[0]
    dma = pltpu.SemaphoreType.DMA
    return pl.pallas_call(
        functools.partial(deal_kernel, n),
        out_shape=jax.ShapeDtypeStruct(payload.shape, payload.dtype),
        in_specs=[pl.BlockSpec(memory_space=pltpu.VMEM)],
        out_specs=pl.BlockSpec(memory_space=pltpu.VMEM),
        scratch_shapes=[dma((n,)), dma((n,)), dma],
        compiler_params=pltpu.CompilerParams(collective_id=1, has_side_effects=True),
        name="deal",
    )(payload)


def layer_norm(block, gain):
    values_in = block.astype(jnp.float32)
    mean = jnp.mean(values_in, axis=-1, keepdims=True)
    var = jnp.mean((values_in - mean) ** 2, axis=-1, keepdims=True)
    return ((values_in - mean) * lax.rsqrt(var + 1e-05) * gain).astype(jnp.bfloat16)


def two_parts(value):
    high = lax.reduce_precision(value, 8, 7)
    return high, lax.reduce_precision(value - high, 8, 7)


def on_device(stem, norm_gain, qkv_weight, segment_ids, dec_queries, stretch_mask):
    rows, width = stem.shape
    heads = width // HD
    scale = HD ** (-0.5)
    tokens_dev = dec_queries.shape[0]
    n_tm = lax.axis_size("tm")
    device = lax.axis_index("tm")
    small = jnp.concatenate(
        [
            dec_queries.reshape(-1),
            stretch_mask.astype(jnp.bfloat16).reshape(-1),
            (segment_ids % 128).astype(jnp.bfloat16),
            (segment_ids // 128).astype(jnp.bfloat16),
        ]
    )
    cuts = [tokens_dev * width, tokens_dev * (width + n_tm)]
    cuts += [cuts[1] + rows, cuts[1] + 2 * rows]
    depth, columns = qkv_weight.shape
    small = jnp.pad(small, (0, -cuts[3] % columns)).reshape(-1, columns)
    gathered, halo = gather(jnp.concatenate([qkv_weight, small], axis=0), stem, n_tm)
    weight = gathered[:, :depth].reshape(n_tm * depth, columns)
    small_all = gathered[:, depth:].reshape(n_tm, -1)
    all_queries = small_all[:, : cuts[0]].reshape(n_tm * tokens_dev, width)
    all_masks = small_all[:, cuts[0] : cuts[1]].reshape(n_tm * tokens_dev, n_tm)
    seg_low = small_all[:, cuts[1] : cuts[2]].reshape(-1).astype(jnp.int32)
    seg_high = small_all[:, cuts[2] : cuts[3]].reshape(-1).astype(jnp.int32)
    around = halo.shape[0]
    seg_all = jnp.pad(seg_high * 128 + seg_low, (2 * REACH * rows, 2 * REACH * rows))
    chip = device // 2
    seg_wide = lax.dynamic_slice_in_dim(seg_all, chip * 2 * rows, around * rows, 0)
    block_at = chip * 2 - 2 * REACH + jnp.arange(around, dtype=jnp.int32)
    exists = (block_at >= 0) & (block_at < n_tm)
    halo = jnp.where(exists[:, None, None], halo, jnp.bfloat16(0)).reshape(around * rows, width)
    query_part = jnp.dot(
        layer_norm(stem, norm_gain), weight[:, :width], preferred_element_type=jnp.float32
    ).astype(jnp.bfloat16)
    extended = jnp.dot(
        layer_norm(halo, norm_gain), weight[:, width:], preferred_element_type=jnp.float32
    ).astype(jnp.bfloat16)
    same = segment_ids[:, None] == seg_wide[None, :]
    group = math.gcd(heads, 4)
    span = group * HD
    groups = heads // group

    def attend(index):
        start = index * span
        query_group = lax.dynamic_slice_in_dim(query_part, start, span, 1).reshape(rows, group, HD)
        key_group = lax.dynamic_slice_in_dim(extended, start, span, 1).reshape(-1, group, HD)
        value_group = lax.dynamic_slice_in_dim(extended, width + start, span, 1).reshape(
            -1, group, HD
        )
        scores = (
            jnp.einsum("qhd,khd->hqk", query_group, key_group, preferred_element_type=jnp.float32)
            * scale
        )
        scores = jnp.where(same[None], scores, jnp.float32(-1e30))
        top = jnp.max(scores, axis=-1, keepdims=True)
        raised = jnp.exp(scores - top)
        probs = (raised / jnp.sum(raised, axis=-1, keepdims=True)).astype(jnp.bfloat16)
        context = jnp.einsum("hqk,khd->qhd", probs, value_group, preferred_element_type=jnp.float32)
        return context.reshape(rows, span)

    contexts = lax.map(attend, jnp.arange(groups, dtype=jnp.int32))
    context = jnp.transpose(contexts, (1, 0, 2)).reshape(rows, width)
    memory = (stem.astype(jnp.float32) + context).astype(jnp.bfloat16)
    total_tokens = all_queries.shape[0]
    column = lax.dynamic_slice_in_dim(all_masks, device, 1, 1)[:, 0]
    owner = jnp.arange(total_tokens, dtype=jnp.int32) // tokens_dev
    allowed = (column == 1) | (owner == device)
    query_heads = all_queries.reshape(total_tokens, heads, HD)
    memory_heads = memory.reshape(rows, heads, HD)
    cross = (
        jnp.einsum("thd,phd->htp", query_heads, memory_heads, preferred_element_type=jnp.float32)
        * scale
    )
    top_high, top_low = two_parts(jnp.max(cross, axis=-1))
    shift = top_high + top_low
    weights = jnp.where(
        allowed[None, :, None], jnp.exp(cross - shift[:, :, None]), jnp.float32(0.0)
    )
    den_high, den_low = two_parts(jnp.sum(weights, axis=-1))
    numer = jnp.einsum(
        "htp,phd->thd",
        weights.astype(jnp.bfloat16),
        memory_heads,
        preferred_element_type=jnp.float32,
    ).astype(jnp.bfloat16)
    top_high = jnp.where(allowed[None, :], top_high, jnp.float32(-1e30))
    top_low = jnp.where(allowed[None, :], top_low, jnp.float32(0.0))
    stats = jnp.stack([top_high, top_low, den_high, den_low]).astype(jnp.bfloat16)
    stats = jnp.transpose(stats, (2, 0, 1)).reshape(n_tm, -1)
    payload = jnp.concatenate([numer.reshape(n_tm, -1), stats], axis=1)
    payload = jnp.pad(payload, ((0, 0), (0, -payload.shape[1] % 2048)))
    got = deal(payload.reshape(n_tm, -1, 128)).reshape(n_tm, -1).astype(jnp.float32)
    num_all = got[:, : tokens_dev * width].reshape(n_tm, tokens_dev, heads, HD)
    stats = got[:, tokens_dev * width : tokens_dev * (width + 4 * heads)]
    stats = stats.reshape(n_tm, tokens_dev, 4, heads)
    top_all = stats[:, :, 0] + stats[:, :, 1]
    den_all = stats[:, :, 2] + stats[:, :, 3]
    best = jnp.max(top_all, axis=0)
    factor = jnp.exp(top_all - best[None])
    num_total = jnp.sum(factor[..., None] * num_all, axis=0)
    den_total = jnp.sum(factor * den_all, axis=0)
    cross_out = (num_total / den_total[..., None]).reshape(tokens_dev, width).astype(jnp.bfloat16)
    return (memory, cross_out)


def solution(mesh):
    placed = (
        P(("utt", "tm"), None),
        P(),
        P("tm", None),
        P(("utt", "tm")),
        P(("utt", "tm"), None),
        P(("utt", "tm"), None),
    )
    return jax.shard_map(
        on_device,
        mesh=mesh,
        in_specs=placed,
        out_specs=(P(("utt", "tm"), None), P(("utt", "tm"), None)),
        check_vma=False,
    )
```

```python
import functools

import jax
import jax.numpy as jnp
from jax import lax
from jax.experimental import pallas as pl
from jax.experimental.pallas import tpu as pltpu
from jax.sharding import PartitionSpec as P

HD = 64
NZ = 8
REACH = 2
MESH = pl.DeviceIdType.MESH


def gather_kernel(nx, w_ref, stem_ref, wide_ref, halo_ref, w_recv, w_zs, w_xs, w_ps, h_recv, h_zs, h_ps, own_sem):
    me = lax.axis_index("tm")
    core = lax.rem(me, 2)
    chip = me // 2
    z = lax.rem(chip, NZ)
    x = chip // NZ
    chips = nx * NZ

    def index(xx, zz):
        return (xx * NZ + zz) * 2 + core

    right_x, left_x, far_x = lax.rem(x + 1, nx), lax.rem(x + nx - 1, nx), lax.rem(x + 2, nx)
    right, left = index(right_x, z), index(left_x, z)
    partner = me + 1 - 2 * core
    up, down = me + 2, me - 2
    has_up, has_down = z < NZ - 1, z > 0
    has_next, has_prev = chip < chips - 1, chip > 0

    barrier = pltpu.get_barrier_semaphore()

    def greet(peer):
        pl.semaphore_signal(barrier, inc=1, device_id={"tm": peer}, device_id_type=MESH)

    greet(right)
    greet(left)
    greet(partner)

    @pl.when(has_next)
    def _():
        greet(up)

    @pl.when(has_prev)
    def _():
        greet(down)

    pl.semaphore_wait(barrier, 3 + has_next.astype(jnp.int32) + has_prev.astype(jnp.int32))

    def w_copy(shard, peer, send_sem, own=False):
        return pltpu.make_async_remote_copy(
            src_ref=w_ref if own else wide_ref.at[shard],
            dst_ref=wide_ref.at[shard],
            send_sem=send_sem,
            recv_sem=w_recv.at[shard],
            device_id={"tm": peer},
            device_id_type=MESH,
        )

    def h_copy(from_slot, to_slot, peer, send_sem, own=False):
        return pltpu.make_async_remote_copy(
            src_ref=stem_ref if own else halo_ref.at[from_slot],
            dst_ref=halo_ref.at[to_slot],
            send_sem=send_sem,
            recv_sem=h_recv.at[to_slot],
            device_id={"tm": peer},
            device_id_type=MESH,
        )

    def to_right(xx, zz, slot, own=False):
        return w_copy(index(xx, zz), right, w_xs.at[0, slot * NZ + zz], own)

    def to_left(xx, zz, slot, own=False):
        return w_copy(index(xx, zz), left, w_xs.at[1, slot * NZ + zz], own)

    def to_partner(xx, zz, own=False):
        return w_copy(index(xx, zz), partner, w_ps.at[xx * NZ + zz], own)

    def to_up(zz, own=False):
        return w_copy(index(x, zz), up, w_zs.at[0, zz], own)

    def to_down(zz, own=False):
        return w_copy(index(x, zz), down, w_zs.at[1, zz], own)

    def slot_of(step, cc):
        return (step + REACH) * 2 + cc

    own_slot = slot_of(0, core)
    h_next = h_copy(own_slot, slot_of(-1, core), up, h_zs.at[0], True)
    h_prev = h_copy(own_slot, slot_of(1, core), down, h_zs.at[1], True)
    h_own = h_copy(own_slot, own_slot, partner, h_ps.at[2], True)
    relay_next = h_copy(slot_of(-1, core), slot_of(-2, core), up, h_zs.at[2])
    relay_prev = h_copy(slot_of(1, core), slot_of(2, core), down, h_zs.at[3])

    def h_pass(step):
        slot = slot_of(step, core)
        return h_copy(slot, slot, partner, h_ps.at[step + REACH])

    def w_arrived(shard):
        pltpu.make_async_copy(wide_ref.at[shard], wide_ref.at[shard], w_recv.at[shard]).wait()

    def h_arrived(slot):
        pltpu.make_async_copy(halo_ref.at[slot], halo_ref.at[slot], h_recv.at[slot]).wait()

    @pl.when(has_up)
    def _():
        to_up(z, True).start()

    @pl.when(has_down)
    def _():
        to_down(z, True).start()

    @pl.when(has_next)
    def _():
        h_next.start()

    @pl.when(has_prev)
    def _():
        h_prev.start()

    to_right(x, z, 0, True).start()
    to_left(x, z, 0, True).start()
    to_partner(x, z, True).start()
    h_own.start()
    own_w = pltpu.make_async_copy(w_ref, wide_ref.at[me], own_sem.at[0])
    own_h = pltpu.make_async_copy(stem_ref, halo_ref.at[own_slot], own_sem.at[1])
    own_w.start()
    own_h.start()

    def beside(zz, fresh):
        ok = (zz >= 0) & (zz < NZ) & fresh

        @pl.when(ok)
        def _():
            even = lax.rem(zz, 2) == 0
            w_arrived(index(left_x, zz))
            to_partner(left_x, zz).start()

            @pl.when(even)
            def _():
                to_right(left_x, zz, 1).start()

            w_arrived(index(right_x, zz))
            to_partner(right_x, zz).start()

            @pl.when(jnp.logical_not(even))
            def _():
                to_left(right_x, zz, 1).start()

    def far(zz, fresh):
        @pl.when((zz >= 0) & (zz < NZ) & fresh)
        def _():
            w_arrived(index(far_x, zz))
            to_partner(far_x, zz).start()

    def step(s, carry):
        below, above = z - s, z + s

        @pl.when((below >= 0) & (s > 0) & (s < NZ))
        def _():
            w_arrived(index(x, below))

            @pl.when(has_up)
            def _():
                to_up(below).start()

            to_right(x, below, 0).start()
            to_left(x, below, 0).start()
            to_partner(x, below).start()

        @pl.when((above < NZ) & (s > 0))
        def _():
            w_arrived(index(x, above))

            @pl.when(has_down)
            def _():
                to_down(above).start()

            to_right(x, above, 0).start()
            to_left(x, above, 0).start()
            to_partner(x, above).start()

        beside(z - (s - 1), s >= 1)
        beside(z + (s - 1), s >= 2)
        far(z - (s - 2), s >= 2)
        far(z + (s - 2), s >= 3)
        return carry

    lax.fori_loop(1, 4, step, 0)

    @pl.when(has_prev)
    def _():
        h_arrived(slot_of(-1, core))
        h_pass(-1).start()

        @pl.when(has_next)
        def _():
            relay_next.start()

    @pl.when(has_next)
    def _():
        h_arrived(slot_of(1, core))
        h_pass(1).start()

        @pl.when(has_prev)
        def _():
            relay_prev.start()

    lax.fori_loop(4, NZ + 2, step, 0)

    @pl.when(chip >= 2)
    def _():
        h_arrived(slot_of(-2, core))
        h_pass(-2).start()

    @pl.when(chip < chips - 2)
    def _():
        h_arrived(slot_of(2, core))
        h_pass(2).start()

    def settle(i, carry):
        w_arrived(i * 2 + 1 - core)
        to_partner(i // NZ, lax.rem(i, NZ), False).wait_send()
        return carry

    lax.fori_loop(0, chips, settle, 0)

    def settle_z(zz, carry):
        @pl.when((zz <= z) & has_up)
        def _():
            to_up(zz).wait_send()

        @pl.when((zz >= z) & has_down)
        def _():
            to_down(zz).wait_send()

        to_right(x, zz, 0).wait_send()
        to_left(x, zz, 0).wait_send()
        even = lax.rem(zz, 2) == 0

        @pl.when(even)
        def _():
            to_right(left_x, zz, 1).wait_send()

        @pl.when(jnp.logical_not(even))
        def _():
            to_left(right_x, zz, 1).wait_send()

        return carry

    lax.fori_loop(0, NZ, settle_z, 0)

    def other(step):
        h_arrived(slot_of(step, 1 - core))

    other(0)
    h_own.wait_send()

    @pl.when(has_next)
    def _():
        h_next.wait_send()
        h_pass(1).wait_send()
        other(1)

    @pl.when(has_prev)
    def _():
        h_prev.wait_send()
        h_pass(-1).wait_send()
        other(-1)

    @pl.when(has_next & has_prev)
    def _():
        relay_next.wait_send()
        relay_prev.wait_send()

    @pl.when(chip >= 2)
    def _():
        h_pass(-2).wait_send()
        other(-2)

    @pl.when(chip < chips - 2)
    def _():
        h_pass(2).wait_send()
        other(2)

    own_w.wait()
    own_h.wait()


def gather(wide, stem, n_tm):
    nx = n_tm // (2 * NZ)
    dma = pltpu.SemaphoreType.DMA
    return pl.pallas_call(
        functools.partial(gather_kernel, nx),
        out_shape=(
            jax.ShapeDtypeStruct((n_tm, *wide.shape), wide.dtype),
            jax.ShapeDtypeStruct((4 * REACH + 2, *stem.shape), stem.dtype),
        ),
        in_specs=[pl.BlockSpec(memory_space=pltpu.VMEM)] * 2,
        out_specs=(pl.BlockSpec(memory_space=pl.ANY), pl.BlockSpec(memory_space=pl.ANY)),
        scratch_shapes=[
            dma((n_tm,)),
            dma((2, NZ)),
            dma((2, 2 * NZ)),
            dma((n_tm // 2,)),
            dma((4 * REACH + 2,)),
            dma((4,)),
            dma((2 * REACH + 1,)),
            dma((2,)),
        ],
        compiler_params=pltpu.CompilerParams(collective_id=0, has_side_effects=True),
        name="gather",
    )(wide, stem)


def deal_kernel(n, out_ref, in_ref, send_sem, recv_sem, own_sem):
    me = lax.axis_index("tm")
    barrier = pltpu.get_barrier_semaphore()

    def peer_of(i):
        return lax.rem(me + i, n)

    def greet(i, carry):
        pl.semaphore_signal(barrier, inc=1, device_id={"tm": peer_of(i)}, device_id_type=MESH)
        return carry

    lax.fori_loop(1, n, greet, 0)
    own = pltpu.make_async_copy(out_ref.at[me], in_ref.at[me], own_sem)
    own.start()
    pl.semaphore_wait(barrier, n - 1)

    def copy(i):
        peer = peer_of(i)
        return pltpu.make_async_remote_copy(
            src_ref=out_ref.at[peer],
            dst_ref=in_ref.at[me],
            send_sem=send_sem.at[i],
            recv_sem=recv_sem.at[me],
            device_id={"tm": peer},
            device_id_type=MESH,
        )

    def send(i, carry):
        copy(i).start()
        return carry

    lax.fori_loop(1, n, send, 0)
    own.wait()

    def settle(i, carry):
        peer = peer_of(i)
        pltpu.make_async_copy(in_ref.at[peer], in_ref.at[peer], recv_sem.at[peer]).wait()
        copy(i).wait_send()
        return carry

    lax.fori_loop(1, n, settle, 0)


def deal(payload):
    n = payload.shape[0]
    dma = pltpu.SemaphoreType.DMA
    return pl.pallas_call(
        functools.partial(deal_kernel, n),
        out_shape=jax.ShapeDtypeStruct(payload.shape, payload.dtype),
        in_specs=[pl.BlockSpec(memory_space=pltpu.VMEM)],
        out_specs=pl.BlockSpec(memory_space=pltpu.VMEM),
        scratch_shapes=[dma((n,)), dma((n,)), dma],
        compiler_params=pltpu.CompilerParams(collective_id=1, has_side_effects=True),
        name="deal",
    )(payload)


def encode_kernel(heads_step, own_ref, halo_ref, exists_ref, wq_ref, wk_ref, wv_ref, bias_ref, stem_ref, out_ref, clean):
    @pl.when(pl.program_id(0) == 0)
    def _():
        clean[...] = jnp.where(exists_ref[...] > 0, halo_ref[...], jnp.bfloat16(0))

    def project(rows, w_ref):
        return jnp.dot(rows, w_ref[...], preferred_element_type=jnp.float32).astype(jnp.bfloat16)

    query = project(own_ref[...], wq_ref) * jnp.bfloat16(HD ** (-0.5))
    key = project(clean[...], wk_ref)
    value = project(clean[...], wv_ref)
    pair = 2 * HD
    low = lax.broadcasted_iota(jnp.int32, (query.shape[0], pair), 1) < HD
    for p in range(heads_step // 2):
        at = slice(p * pair, (p + 1) * pair)
        parts = []
        for h in range(2):
            mine = low if h == 0 else jnp.logical_not(low)
            scores = lax.dot_general(
                jnp.where(mine, query[:, at], jnp.bfloat16(0)),
                key[:, at],
                (((1,), (1,)), ((), ())),
                preferred_element_type=jnp.float32,
            )
            scores = scores + bias_ref[...]
            raised = jnp.exp(scores - jnp.max(scores, axis=-1, keepdims=True))
            total = jnp.sum(raised, axis=-1, keepdims=True)
            probs = (raised * (1.0 / total)).astype(jnp.bfloat16)
            parts.append(jnp.dot(probs, value[:, at], preferred_element_type=jnp.float32))
        context = jnp.where(low, parts[0], parts[1])
        out_ref[:, at] = (stem_ref[:, at].astype(jnp.float32) + context).astype(jnp.bfloat16)


def encode(own, halo, exists, weight, bias, stem):
    rows, width = stem.shape
    depth = own.shape[1]
    around = halo.shape[0]
    heads_step = 4
    span = heads_step * HD
    steps = width // span

    def whole(*shape):
        return pl.BlockSpec(shape, lambda i: (0,) * len(shape))

    def columns(first):
        return pl.BlockSpec((depth, span), lambda i: (0, first * steps + i))

    piece = pl.BlockSpec((rows, span), lambda i: (0, i))
    return pl.pallas_call(
        functools.partial(encode_kernel, heads_step),
        grid=(steps,),
        out_shape=jax.ShapeDtypeStruct(stem.shape, stem.dtype),
        in_specs=[
            whole(rows, depth),
            whole(around, depth),
            whole(around, 1),
            columns(0),
            columns(1),
            columns(2),
            whole(rows, around),
            piece,
        ],
        out_specs=piece,
        scratch_shapes=[pltpu.VMEM((around, depth), jnp.bfloat16)],
        name="encode",
    )(own, halo, exists, weight, weight, weight, bias, stem)


def layer_norm(block, gain):
    values_in = block.astype(jnp.float32)
    mean = jnp.mean(values_in, axis=-1, keepdims=True)
    var = jnp.mean((values_in - mean) ** 2, axis=-1, keepdims=True)
    return ((values_in - mean) * lax.rsqrt(var + 1e-05) * gain).astype(jnp.bfloat16)


def two_parts(value):
    high = lax.reduce_precision(value, 8, 7)
    return high, lax.reduce_precision(value - high, 8, 7)


def on_device(stem, norm_gain, qkv_weight, segment_ids, dec_queries, stretch_mask):
    rows, width = stem.shape
    heads = width // HD
    scale = HD ** (-0.5)
    tokens_dev = dec_queries.shape[0]
    n_tm = lax.axis_size("tm")
    device = lax.axis_index("tm")
    small = jnp.concatenate(
        [
            dec_queries.reshape(-1),
            stretch_mask.astype(jnp.bfloat16).reshape(-1),
            (segment_ids % 128).astype(jnp.bfloat16),
            (segment_ids // 128).astype(jnp.bfloat16),
        ]
    )
    cuts = [tokens_dev * width, tokens_dev * (width + n_tm)]
    cuts += [cuts[1] + rows, cuts[1] + 2 * rows]
    depth, columns = qkv_weight.shape
    padded = depth + 1 + (-(depth + 1) % 8)
    spread_at = (jnp.arange(width) // depth) * padded + jnp.arange(width) % depth
    spread = (spread_at[:, None] == jnp.arange(n_tm * padded)[None, :]).astype(jnp.bfloat16)
    own = jnp.dot(
        layer_norm(stem, norm_gain), spread, preferred_element_type=jnp.float32
    ).astype(jnp.bfloat16)
    small = jnp.pad(small, (0, (padded - depth) * columns - cuts[3])).reshape(-1, columns)
    gathered, halo = gather(jnp.concatenate([qkv_weight, small], axis=0), own, n_tm)
    weight = gathered.reshape(n_tm * padded, columns)
    small_all = gathered[:, depth]
    all_queries = small_all[:, : cuts[0]].reshape(n_tm * tokens_dev, width)
    all_masks = small_all[:, cuts[0] : cuts[1]].reshape(n_tm * tokens_dev, n_tm)
    seg_low = small_all[:, cuts[1] : cuts[2]].reshape(-1).astype(jnp.int32)
    seg_high = small_all[:, cuts[2] : cuts[3]].reshape(-1).astype(jnp.int32)
    around = halo.shape[0]
    seg_all = jnp.pad(seg_high * 128 + seg_low, (2 * REACH * rows, 2 * REACH * rows))
    chip = device // 2
    seg_wide = lax.dynamic_slice_in_dim(seg_all, chip * 2 * rows, around * rows, 0)
    block_at = chip * 2 - 2 * REACH + jnp.arange(around, dtype=jnp.int32)
    exists = (block_at >= 0) & (block_at < n_tm)
    exists = jnp.repeat(exists.astype(jnp.int32), rows)[:, None]
    same = segment_ids[:, None] == seg_wide[None, :]
    bias = jnp.where(same, jnp.float32(0.0), jnp.float32(-1e30))
    memory = encode(own, halo.reshape(around * rows, -1), exists, weight, bias, stem)
    total_tokens = all_queries.shape[0]
    column = lax.dynamic_slice_in_dim(all_masks, device, 1, 1)[:, 0]
    owner = jnp.arange(total_tokens, dtype=jnp.int32) // tokens_dev
    allowed = (column == 1) | (owner == device)
    query_heads = all_queries.reshape(total_tokens, heads, HD)
    memory_heads = memory.reshape(rows, heads, HD)
    cross = (
        jnp.einsum("thd,phd->htp", query_heads, memory_heads, preferred_element_type=jnp.float32)
        * scale
    )
    top_high, top_low = two_parts(jnp.max(cross, axis=-1))
    shift = top_high + top_low
    weights = jnp.where(
        allowed[None, :, None], jnp.exp(cross - shift[:, :, None]), jnp.float32(0.0)
    )
    den_high, den_low = two_parts(jnp.sum(weights, axis=-1))
    numer = jnp.einsum(
        "htp,phd->thd",
        weights.astype(jnp.bfloat16),
        memory_heads,
        preferred_element_type=jnp.float32,
    ).astype(jnp.bfloat16)
    top_high = jnp.where(allowed[None, :], top_high, jnp.float32(-1e30))
    top_low = jnp.where(allowed[None, :], top_low, jnp.float32(0.0))
    stats = jnp.stack([top_high, top_low, den_high, den_low]).astype(jnp.bfloat16)
    stats = jnp.transpose(stats, (2, 0, 1)).reshape(n_tm, -1)
    payload = jnp.concatenate([numer.reshape(n_tm, -1), stats], axis=1)
    payload = jnp.pad(payload, ((0, 0), (0, -payload.shape[1] % 2048)))
    got = deal(payload.reshape(n_tm, -1, 128)).reshape(n_tm, -1).astype(jnp.float32)
    num_all = got[:, : tokens_dev * width].reshape(n_tm, tokens_dev, heads, HD)
    stats = got[:, tokens_dev * width : tokens_dev * (width + 4 * heads)]
    stats = stats.reshape(n_tm, tokens_dev, 4, heads)
    top_all = stats[:, :, 0] + stats[:, :, 1]
    den_all = stats[:, :, 2] + stats[:, :, 3]
    best = jnp.max(top_all, axis=0)
    factor = jnp.exp(top_all - best[None])
    num_total = jnp.sum(factor[..., None] * num_all, axis=0)
    den_total = jnp.sum(factor * den_all, axis=0)
    cross_out = (num_total / den_total[..., None]).reshape(tokens_dev, width).astype(jnp.bfloat16)
    return (memory, cross_out)


def solution(mesh):
    placed = (
        P(("utt", "tm"), None),
        P(),
        P("tm", None),
        P(("utt", "tm")),
        P(("utt", "tm"), None),
        P(("utt", "tm"), None),
    )
    return jax.shard_map(
        on_device,
        mesh=mesh,
        in_specs=placed,
        out_specs=(P(("utt", "tm"), None), P(("utt", "tm"), None)),
        check_vma=False,
    )
```

```python
import functools

import jax
import jax.numpy as jnp
from jax import lax
from jax.experimental import pallas as pl
from jax.experimental.pallas import tpu as pltpu
from jax.sharding import PartitionSpec as P

HD = 64
NZ = 8
REACH = 2
MESH = pl.DeviceIdType.MESH


def gather_kernel(nx, w_ref, stem_ref, wide_ref, halo_ref, w_recv, w_zs, w_xs, w_ps, h_recv, h_zs, h_ps, own_sem):
    me = lax.axis_index("tm")
    core = lax.rem(me, 2)
    chip = me // 2
    z = lax.rem(chip, NZ)
    x = chip // NZ
    chips = nx * NZ

    def index(xx, zz):
        return (xx * NZ + zz) * 2 + core

    right_x, left_x, far_x = lax.rem(x + 1, nx), lax.rem(x + nx - 1, nx), lax.rem(x + 2, nx)
    right, left = index(right_x, z), index(left_x, z)
    partner = me + 1 - 2 * core
    up, down = me + 2, me - 2
    has_up, has_down = z < NZ - 1, z > 0
    has_next, has_prev = chip < chips - 1, chip > 0

    barrier = pltpu.get_barrier_semaphore()

    def greet(peer):
        pl.semaphore_signal(barrier, inc=1, device_id={"tm": peer}, device_id_type=MESH)

    greet(right)
    greet(left)
    greet(partner)

    @pl.when(has_next)
    def _():
        greet(up)

    @pl.when(has_prev)
    def _():
        greet(down)

    pl.semaphore_wait(barrier, 3 + has_next.astype(jnp.int32) + has_prev.astype(jnp.int32))

    def w_copy(shard, peer, send_sem, own=False):
        return pltpu.make_async_remote_copy(
            src_ref=w_ref if own else wide_ref.at[shard],
            dst_ref=wide_ref.at[shard],
            send_sem=send_sem,
            recv_sem=w_recv.at[shard],
            device_id={"tm": peer},
            device_id_type=MESH,
        )

    def h_copy(from_slot, to_slot, peer, send_sem, own=False):
        return pltpu.make_async_remote_copy(
            src_ref=stem_ref if own else halo_ref.at[from_slot],
            dst_ref=halo_ref.at[to_slot],
            send_sem=send_sem,
            recv_sem=h_recv.at[to_slot],
            device_id={"tm": peer},
            device_id_type=MESH,
        )

    def to_right(xx, zz, slot, own=False):
        return w_copy(index(xx, zz), right, w_xs.at[0, slot * NZ + zz], own)

    def to_left(xx, zz, slot, own=False):
        return w_copy(index(xx, zz), left, w_xs.at[1, slot * NZ + zz], own)

    def to_partner(xx, zz, own=False):
        return w_copy(index(xx, zz), partner, w_ps.at[xx * NZ + zz], own)

    def to_up(zz, own=False):
        return w_copy(index(x, zz), up, w_zs.at[0, zz], own)

    def to_down(zz, own=False):
        return w_copy(index(x, zz), down, w_zs.at[1, zz], own)

    def slot_of(step, cc):
        return (step + REACH) * 2 + cc

    own_slot = slot_of(0, core)
    h_next = h_copy(own_slot, slot_of(-1, core), up, h_zs.at[0], True)
    h_prev = h_copy(own_slot, slot_of(1, core), down, h_zs.at[1], True)
    h_own = h_copy(own_slot, own_slot, partner, h_ps.at[2], True)
    relay_next = h_copy(slot_of(-1, core), slot_of(-2, core), up, h_zs.at[2])
    relay_prev = h_copy(slot_of(1, core), slot_of(2, core), down, h_zs.at[3])

    def h_pass(step):
        slot = slot_of(step, core)
        return h_copy(slot, slot, partner, h_ps.at[step + REACH])

    def w_arrived(shard):
        pltpu.make_async_copy(wide_ref.at[shard], wide_ref.at[shard], w_recv.at[shard]).wait()

    def h_arrived(slot):
        pltpu.make_async_copy(halo_ref.at[slot], halo_ref.at[slot], h_recv.at[slot]).wait()

    @pl.when(has_up)
    def _():
        to_up(z, True).start()

    @pl.when(has_down)
    def _():
        to_down(z, True).start()

    to_right(x, z, 0, True).start()
    to_left(x, z, 0, True).start()
    to_partner(x, z, True).start()
    h_own.start()
    own_w = pltpu.make_async_copy(w_ref, wide_ref.at[me], own_sem.at[0])
    own_h = pltpu.make_async_copy(stem_ref, halo_ref.at[own_slot], own_sem.at[1])
    own_w.start()
    own_h.start()

    def beside(zz, fresh):
        ok = (zz >= 0) & (zz < NZ) & fresh

        @pl.when(ok)
        def _():
            even = lax.rem(zz, 2) == 0
            w_arrived(index(left_x, zz))
            to_partner(left_x, zz).start()

            @pl.when(even)
            def _():
                to_right(left_x, zz, 1).start()

            w_arrived(index(right_x, zz))
            to_partner(right_x, zz).start()

            @pl.when(jnp.logical_not(even))
            def _():
                to_left(right_x, zz, 1).start()

    def far(zz, fresh):
        @pl.when((zz >= 0) & (zz < NZ) & fresh)
        def _():
            w_arrived(index(far_x, zz))
            to_partner(far_x, zz).start()

    def step(s, carry):
        below, above = z - s, z + s

        @pl.when((below >= 0) & (s > 0) & (s < NZ))
        def _():
            w_arrived(index(x, below))

            @pl.when(has_up)
            def _():
                to_up(below).start()

            to_right(x, below, 0).start()
            to_left(x, below, 0).start()
            to_partner(x, below).start()

        @pl.when((above < NZ) & (s > 0))
        def _():
            w_arrived(index(x, above))

            @pl.when(has_down)
            def _():
                to_down(above).start()

            to_right(x, above, 0).start()
            to_left(x, above, 0).start()
            to_partner(x, above).start()

        beside(z - (s - 1), s >= 1)
        beside(z + (s - 1), s >= 2)
        far(z - (s - 2), s >= 2)
        far(z + (s - 2), s >= 3)
        return carry

    lax.fori_loop(1, 4, step, 0)

    @pl.when(has_next)
    def _():
        h_next.start()

    @pl.when(has_prev)
    def _():
        h_prev.start()

    lax.fori_loop(4, NZ, step, 0)

    @pl.when(has_prev)
    def _():
        h_arrived(slot_of(-1, core))
        h_pass(-1).start()

        @pl.when(has_next)
        def _():
            relay_next.start()

    @pl.when(has_next)
    def _():
        h_arrived(slot_of(1, core))
        h_pass(1).start()

        @pl.when(has_prev)
        def _():
            relay_prev.start()

    lax.fori_loop(NZ, NZ + 2, step, 0)

    @pl.when(chip >= 2)
    def _():
        h_arrived(slot_of(-2, core))
        h_pass(-2).start()

    @pl.when(chip < chips - 2)
    def _():
        h_arrived(slot_of(2, core))
        h_pass(2).start()

    def settle(i, carry):
        w_arrived(i * 2 + 1 - core)
        to_partner(i // NZ, lax.rem(i, NZ), False).wait_send()
        return carry

    lax.fori_loop(0, chips, settle, 0)

    def settle_z(zz, carry):
        @pl.when((zz <= z) & has_up)
        def _():
            to_up(zz).wait_send()

        @pl.when((zz >= z) & has_down)
        def _():
            to_down(zz).wait_send()

        to_right(x, zz, 0).wait_send()
        to_left(x, zz, 0).wait_send()
        even = lax.rem(zz, 2) == 0

        @pl.when(even)
        def _():
            to_right(left_x, zz, 1).wait_send()

        @pl.when(jnp.logical_not(even))
        def _():
            to_left(right_x, zz, 1).wait_send()

        return carry

    lax.fori_loop(0, NZ, settle_z, 0)

    def other(step):
        h_arrived(slot_of(step, 1 - core))

    other(0)
    h_own.wait_send()

    @pl.when(has_next)
    def _():
        h_next.wait_send()
        h_pass(1).wait_send()
        other(1)

    @pl.when(has_prev)
    def _():
        h_prev.wait_send()
        h_pass(-1).wait_send()
        other(-1)

    @pl.when(has_next & has_prev)
    def _():
        relay_next.wait_send()
        relay_prev.wait_send()

    @pl.when(chip >= 2)
    def _():
        h_pass(-2).wait_send()
        other(-2)

    @pl.when(chip < chips - 2)
    def _():
        h_pass(2).wait_send()
        other(2)

    own_w.wait()
    own_h.wait()


def gather(wide, stem, n_tm):
    nx = n_tm // (2 * NZ)
    dma = pltpu.SemaphoreType.DMA
    return pl.pallas_call(
        functools.partial(gather_kernel, nx),
        out_shape=(
            jax.ShapeDtypeStruct((n_tm, *wide.shape), wide.dtype),
            jax.ShapeDtypeStruct((4 * REACH + 2, *stem.shape), stem.dtype),
        ),
        in_specs=[pl.BlockSpec(memory_space=pltpu.VMEM)] * 2,
        out_specs=(pl.BlockSpec(memory_space=pl.ANY), pl.BlockSpec(memory_space=pl.ANY)),
        scratch_shapes=[
            dma((n_tm,)),
            dma((2, NZ)),
            dma((2, 2 * NZ)),
            dma((n_tm // 2,)),
            dma((4 * REACH + 2,)),
            dma((4,)),
            dma((2 * REACH + 1,)),
            dma((2,)),
        ],
        compiler_params=pltpu.CompilerParams(collective_id=0, has_side_effects=True),
        name="gather",
    )(wide, stem)


def deal_kernel(n, out_ref, in_ref, send_sem, recv_sem, own_sem):
    me = lax.axis_index("tm")
    barrier = pltpu.get_barrier_semaphore()

    def peer_of(i):
        return lax.rem(me + i, n)

    def greet(i, carry):
        pl.semaphore_signal(barrier, inc=1, device_id={"tm": peer_of(i)}, device_id_type=MESH)
        return carry

    lax.fori_loop(1, n, greet, 0)
    own = pltpu.make_async_copy(out_ref.at[me], in_ref.at[me], own_sem)
    own.start()
    pl.semaphore_wait(barrier, n - 1)

    def copy(i):
        peer = peer_of(i)
        return pltpu.make_async_remote_copy(
            src_ref=out_ref.at[peer],
            dst_ref=in_ref.at[me],
            send_sem=send_sem.at[i],
            recv_sem=recv_sem.at[me],
            device_id={"tm": peer},
            device_id_type=MESH,
        )

    def send(i, carry):
        copy(i).start()
        return carry

    lax.fori_loop(1, n, send, 0)
    own.wait()

    def settle(i, carry):
        peer = peer_of(i)
        pltpu.make_async_copy(in_ref.at[peer], in_ref.at[peer], recv_sem.at[peer]).wait()
        copy(i).wait_send()
        return carry

    lax.fori_loop(1, n, settle, 0)


def deal(payload):
    n = payload.shape[0]
    dma = pltpu.SemaphoreType.DMA
    return pl.pallas_call(
        functools.partial(deal_kernel, n),
        out_shape=jax.ShapeDtypeStruct(payload.shape, payload.dtype),
        in_specs=[pl.BlockSpec(memory_space=pltpu.VMEM)],
        out_specs=pl.BlockSpec(memory_space=pltpu.VMEM),
        scratch_shapes=[dma((n,)), dma((n,)), dma],
        compiler_params=pltpu.CompilerParams(collective_id=1, has_side_effects=True),
        name="deal",
    )(payload)


def encode_kernel(heads_step, own_ref, halo_ref, exists_ref, wq_ref, wk_ref, wv_ref, bias_ref, stem_ref, out_ref, clean):
    @pl.when(pl.program_id(0) == 0)
    def _():
        clean[...] = jnp.where(exists_ref[...] > 0, halo_ref[...], jnp.bfloat16(0))

    def project(rows, w_ref):
        return jnp.dot(rows, w_ref[...], preferred_element_type=jnp.float32).astype(jnp.bfloat16)

    query = project(own_ref[...], wq_ref) * jnp.bfloat16(HD ** (-0.5))
    key = project(clean[...], wk_ref)
    value = project(clean[...], wv_ref)
    pair = 2 * HD
    low = lax.broadcasted_iota(jnp.int32, (query.shape[0], pair), 1) < HD
    for p in range(heads_step // 2):
        at = slice(p * pair, (p + 1) * pair)
        parts = []
        for h in range(2):
            mine = low if h == 0 else jnp.logical_not(low)
            scores = lax.dot_general(
                jnp.where(mine, query[:, at], jnp.bfloat16(0)),
                key[:, at],
                (((1,), (1,)), ((), ())),
                preferred_element_type=jnp.float32,
            )
            scores = scores + bias_ref[...]
            raised = jnp.exp(scores - jnp.max(scores, axis=-1, keepdims=True))
            total = jnp.sum(raised, axis=-1, keepdims=True)
            probs = (raised * (1.0 / total)).astype(jnp.bfloat16)
            parts.append(jnp.dot(probs, value[:, at], preferred_element_type=jnp.float32))
        context = jnp.where(low, parts[0], parts[1])
        out_ref[:, at] = (stem_ref[:, at].astype(jnp.float32) + context).astype(jnp.bfloat16)


def encode(own, halo, exists, weight, bias, stem):
    rows, width = stem.shape
    depth = own.shape[1]
    around = halo.shape[0]
    heads_step = 4
    span = heads_step * HD
    steps = width // span

    def whole(*shape):
        return pl.BlockSpec(shape, lambda i: (0,) * len(shape))

    def columns(first):
        return pl.BlockSpec((depth, span), lambda i: (0, first * steps + i))

    piece = pl.BlockSpec((rows, span), lambda i: (0, i))
    return pl.pallas_call(
        functools.partial(encode_kernel, heads_step),
        grid=(steps,),
        out_shape=jax.ShapeDtypeStruct(stem.shape, stem.dtype),
        in_specs=[
            whole(rows, depth),
            whole(around, depth),
            whole(around, 1),
            columns(0),
            columns(1),
            columns(2),
            whole(rows, around),
            piece,
        ],
        out_specs=piece,
        scratch_shapes=[pltpu.VMEM((around, depth), jnp.bfloat16)],
        name="encode",
    )(own, halo, exists, weight, weight, weight, bias, stem)


def layer_norm(block, gain):
    values_in = block.astype(jnp.float32)
    mean = jnp.mean(values_in, axis=-1, keepdims=True)
    var = jnp.mean((values_in - mean) ** 2, axis=-1, keepdims=True)
    return ((values_in - mean) * lax.rsqrt(var + 1e-05) * gain).astype(jnp.bfloat16)


def two_parts(value):
    high = lax.reduce_precision(value, 8, 7)
    return high, lax.reduce_precision(value - high, 8, 7)


def on_device(stem, norm_gain, qkv_weight, segment_ids, dec_queries, stretch_mask):
    rows, width = stem.shape
    heads = width // HD
    scale = HD ** (-0.5)
    tokens_dev = dec_queries.shape[0]
    n_tm = lax.axis_size("tm")
    device = lax.axis_index("tm")
    small = jnp.concatenate(
        [
            dec_queries.reshape(-1),
            stretch_mask.astype(jnp.bfloat16).reshape(-1),
            (segment_ids % 128).astype(jnp.bfloat16),
            (segment_ids // 128).astype(jnp.bfloat16),
        ]
    )
    cuts = [tokens_dev * width, tokens_dev * (width + n_tm)]
    cuts += [cuts[1] + rows, cuts[1] + 2 * rows]
    depth, columns = qkv_weight.shape
    padded = depth + 1 + (-(depth + 1) % 8)
    spread_at = (jnp.arange(width) // depth) * padded + jnp.arange(width) % depth
    spread = (spread_at[:, None] == jnp.arange(n_tm * padded)[None, :]).astype(jnp.bfloat16)
    own = jnp.dot(
        layer_norm(stem, norm_gain), spread, preferred_element_type=jnp.float32
    ).astype(jnp.bfloat16)
    small = jnp.pad(small, (0, (padded - depth) * columns - cuts[3])).reshape(-1, columns)
    gathered, halo = gather(jnp.concatenate([qkv_weight, small], axis=0), own, n_tm)
    weight = gathered.reshape(n_tm * padded, columns)
    small_all = gathered[:, depth]
    all_queries = small_all[:, : cuts[0]].reshape(n_tm * tokens_dev, width)
    all_masks = small_all[:, cuts[0] : cuts[1]].reshape(n_tm * tokens_dev, n_tm)
    seg_low = small_all[:, cuts[1] : cuts[2]].reshape(-1).astype(jnp.int32)
    seg_high = small_all[:, cuts[2] : cuts[3]].reshape(-1).astype(jnp.int32)
    around = halo.shape[0]
    seg_all = jnp.pad(seg_high * 128 + seg_low, (2 * REACH * rows, 2 * REACH * rows))
    chip = device // 2
    seg_wide = lax.dynamic_slice_in_dim(seg_all, chip * 2 * rows, around * rows, 0)
    block_at = chip * 2 - 2 * REACH + jnp.arange(around, dtype=jnp.int32)
    exists = (block_at >= 0) & (block_at < n_tm)
    exists = jnp.repeat(exists.astype(jnp.int32), rows)[:, None]
    same = segment_ids[:, None] == seg_wide[None, :]
    bias = jnp.where(same, jnp.float32(0.0), jnp.float32(-1e30))
    memory = encode(own, halo.reshape(around * rows, -1), exists, weight, bias, stem)
    total_tokens = all_queries.shape[0]
    column = lax.dynamic_slice_in_dim(all_masks, device, 1, 1)[:, 0]
    owner = jnp.arange(total_tokens, dtype=jnp.int32) // tokens_dev
    allowed = (column == 1) | (owner == device)
    query_heads = all_queries.reshape(total_tokens, heads, HD)
    memory_heads = memory.reshape(rows, heads, HD)
    cross = (
        jnp.einsum("thd,phd->htp", query_heads, memory_heads, preferred_element_type=jnp.float32)
        * scale
    )
    top_high, top_low = two_parts(jnp.max(cross, axis=-1))
    shift = top_high + top_low
    weights = jnp.where(
        allowed[None, :, None], jnp.exp(cross - shift[:, :, None]), jnp.float32(0.0)
    )
    den_high, den_low = two_parts(jnp.sum(weights, axis=-1))
    numer = jnp.einsum(
        "htp,phd->thd",
        weights.astype(jnp.bfloat16),
        memory_heads,
        preferred_element_type=jnp.float32,
    ).astype(jnp.bfloat16)
    top_high = jnp.where(allowed[None, :], top_high, jnp.float32(-1e30))
    top_low = jnp.where(allowed[None, :], top_low, jnp.float32(0.0))
    stats = jnp.stack([top_high, top_low, den_high, den_low]).astype(jnp.bfloat16)
    stats = jnp.transpose(stats, (2, 0, 1)).reshape(n_tm, -1)
    payload = jnp.concatenate([numer.reshape(n_tm, -1), stats], axis=1)
    payload = jnp.pad(payload, ((0, 0), (0, -payload.shape[1] % 1024)))
    got = deal(payload.reshape(n_tm, -1, 128)).reshape(n_tm, -1).astype(jnp.float32)
    num_all = got[:, : tokens_dev * width].reshape(n_tm, tokens_dev, heads, HD)
    stats = got[:, tokens_dev * width : tokens_dev * (width + 4 * heads)]
    stats = stats.reshape(n_tm, tokens_dev, 4, heads)
    top_all = stats[:, :, 0] + stats[:, :, 1]
    den_all = stats[:, :, 2] + stats[:, :, 3]
    best = jnp.max(top_all, axis=0)
    factor = jnp.exp(top_all - best[None])
    num_total = jnp.sum(factor[..., None] * num_all, axis=0)
    den_total = jnp.sum(factor * den_all, axis=0)
    cross_out = (num_total / den_total[..., None]).reshape(tokens_dev, width).astype(jnp.bfloat16)
    return (memory, cross_out)


def solution(mesh):
    placed = (
        P(("utt", "tm"), None),
        P(),
        P("tm", None),
        P(("utt", "tm")),
        P(("utt", "tm"), None),
        P(("utt", "tm"), None),
    )
    return jax.shard_map(
        on_device,
        mesh=mesh,
        in_specs=placed,
        out_specs=(P(("utt", "tm"), None), P(("utt", "tm"), None)),
        check_vma=False,
    )
```

```python
import functools

import jax
import jax.numpy as jnp
from jax import lax
from jax.experimental import pallas as pl
from jax.experimental.pallas import tpu as pltpu
from jax.sharding import PartitionSpec as P

HD = 64
NZ = 8
REACH = 2
MESH = pl.DeviceIdType.MESH


def gather_kernel(nx, w_ref, stem_ref, gain_ref, at_ref, wide_ref, halo_ref, own_ref, w_recv, w_zs, w_xs, w_ps, h_recv, h_zs, h_ps, own_sem):
    me = lax.axis_index("tm")
    core = lax.rem(me, 2)
    chip = me // 2
    z = lax.rem(chip, NZ)
    x = chip // NZ
    chips = nx * NZ

    def index(xx, zz):
        return (xx * NZ + zz) * 2 + core

    right_x, left_x, far_x = lax.rem(x + 1, nx), lax.rem(x + nx - 1, nx), lax.rem(x + 2, nx)
    right, left = index(right_x, z), index(left_x, z)
    partner = me + 1 - 2 * core
    up, down = me + 2, me - 2
    has_up, has_down = z < NZ - 1, z > 0
    has_next, has_prev = chip < chips - 1, chip > 0

    barrier = pltpu.get_barrier_semaphore()

    def greet(peer):
        pl.semaphore_signal(barrier, inc=1, device_id={"tm": peer}, device_id_type=MESH)

    greet(right)
    greet(left)
    greet(partner)

    @pl.when(has_next)
    def _():
        greet(up)

    @pl.when(has_prev)
    def _():
        greet(down)

    pl.semaphore_wait(barrier, 3 + has_next.astype(jnp.int32) + has_prev.astype(jnp.int32))

    def w_copy(shard, peer, send_sem, own=False):
        return pltpu.make_async_remote_copy(
            src_ref=w_ref if own else wide_ref.at[shard],
            dst_ref=wide_ref.at[shard],
            send_sem=send_sem,
            recv_sem=w_recv.at[shard],
            device_id={"tm": peer},
            device_id_type=MESH,
        )

    def h_copy(from_slot, to_slot, peer, send_sem, own=False):
        return pltpu.make_async_remote_copy(
            src_ref=own_ref if own else halo_ref.at[from_slot],
            dst_ref=halo_ref.at[to_slot],
            send_sem=send_sem,
            recv_sem=h_recv.at[to_slot],
            device_id={"tm": peer},
            device_id_type=MESH,
        )

    def to_right(xx, zz, slot, own=False):
        return w_copy(index(xx, zz), right, w_xs.at[0, slot * NZ + zz], own)

    def to_left(xx, zz, slot, own=False):
        return w_copy(index(xx, zz), left, w_xs.at[1, slot * NZ + zz], own)

    def to_partner(xx, zz, own=False):
        return w_copy(index(xx, zz), partner, w_ps.at[xx * NZ + zz], own)

    def to_up(zz, own=False):
        return w_copy(index(x, zz), up, w_zs.at[0, zz], own)

    def to_down(zz, own=False):
        return w_copy(index(x, zz), down, w_zs.at[1, zz], own)

    def slot_of(step, cc):
        return (step + REACH) * 2 + cc

    own_slot = slot_of(0, core)
    h_next = h_copy(own_slot, slot_of(-1, core), up, h_zs.at[0], True)
    h_prev = h_copy(own_slot, slot_of(1, core), down, h_zs.at[1], True)
    h_own = h_copy(own_slot, own_slot, partner, h_ps.at[2], True)
    relay_next = h_copy(slot_of(-1, core), slot_of(-2, core), up, h_zs.at[2])
    relay_prev = h_copy(slot_of(1, core), slot_of(2, core), down, h_zs.at[3])

    def h_pass(step):
        slot = slot_of(step, core)
        return h_copy(slot, slot, partner, h_ps.at[step + REACH])

    def w_arrived(shard):
        pltpu.make_async_copy(wide_ref.at[shard], wide_ref.at[shard], w_recv.at[shard]).wait()

    def h_arrived(slot):
        pltpu.make_async_copy(halo_ref.at[slot], halo_ref.at[slot], h_recv.at[slot]).wait()

    @pl.when(has_up)
    def _():
        to_up(z, True).start()

    @pl.when(has_down)
    def _():
        to_down(z, True).start()

    to_right(x, z, 0, True).start()
    to_left(x, z, 0, True).start()
    to_partner(x, z, True).start()
    own_w = pltpu.make_async_copy(w_ref, wide_ref.at[me], own_sem.at[0])
    own_h = pltpu.make_async_copy(own_ref, halo_ref.at[own_slot], own_sem.at[1])
    own_w.start()

    lanes = lax.broadcasted_iota(jnp.int32, (at_ref.shape[0], own_ref.shape[1]), 1)
    spread = jnp.where(lanes == at_ref[...], 1.0, 0.0).astype(jnp.bfloat16)
    own_ref[...] = jnp.dot(
        layer_norm(stem_ref[...], gain_ref[...]), spread, preferred_element_type=jnp.float32
    ).astype(jnp.bfloat16)

    def beside(zz, fresh):
        ok = (zz >= 0) & (zz < NZ) & fresh

        @pl.when(ok)
        def _():
            even = lax.rem(zz, 2) == 0
            w_arrived(index(left_x, zz))
            to_partner(left_x, zz).start()

            @pl.when(even)
            def _():
                to_right(left_x, zz, 1).start()

            w_arrived(index(right_x, zz))
            to_partner(right_x, zz).start()

            @pl.when(jnp.logical_not(even))
            def _():
                to_left(right_x, zz, 1).start()

    def far(zz, fresh):
        @pl.when((zz >= 0) & (zz < NZ) & fresh)
        def _():
            w_arrived(index(far_x, zz))
            to_partner(far_x, zz).start()

    def step(s, carry):
        below, above = z - s, z + s

        @pl.when((below >= 0) & (s > 0) & (s < NZ))
        def _():
            w_arrived(index(x, below))

            @pl.when(has_up)
            def _():
                to_up(below).start()

            to_right(x, below, 0).start()
            to_left(x, below, 0).start()
            to_partner(x, below).start()

        @pl.when((above < NZ) & (s > 0))
        def _():
            w_arrived(index(x, above))

            @pl.when(has_down)
            def _():
                to_down(above).start()

            to_right(x, above, 0).start()
            to_left(x, above, 0).start()
            to_partner(x, above).start()

        beside(z - (s - 1), s >= 1)
        beside(z + (s - 1), s >= 2)
        far(z - (s - 2), s >= 2)
        far(z + (s - 2), s >= 3)
        return carry

    lax.fori_loop(1, 4, step, 0)

    h_own.start()
    own_h.start()

    @pl.when(has_next)
    def _():
        h_next.start()

    @pl.when(has_prev)
    def _():
        h_prev.start()

    lax.fori_loop(4, NZ, step, 0)

    @pl.when(has_prev)
    def _():
        h_arrived(slot_of(-1, core))
        h_pass(-1).start()

        @pl.when(has_next)
        def _():
            relay_next.start()

    @pl.when(has_next)
    def _():
        h_arrived(slot_of(1, core))
        h_pass(1).start()

        @pl.when(has_prev)
        def _():
            relay_prev.start()

    lax.fori_loop(NZ, NZ + 2, step, 0)

    @pl.when(chip >= 2)
    def _():
        h_arrived(slot_of(-2, core))
        h_pass(-2).start()

    @pl.when(chip < chips - 2)
    def _():
        h_arrived(slot_of(2, core))
        h_pass(2).start()

    def settle(i, carry):
        w_arrived(i * 2 + 1 - core)
        to_partner(i // NZ, lax.rem(i, NZ), False).wait_send()
        return carry

    lax.fori_loop(0, chips, settle, 0)

    def settle_z(zz, carry):
        @pl.when((zz <= z) & has_up)
        def _():
            to_up(zz).wait_send()

        @pl.when((zz >= z) & has_down)
        def _():
            to_down(zz).wait_send()

        to_right(x, zz, 0).wait_send()
        to_left(x, zz, 0).wait_send()
        even = lax.rem(zz, 2) == 0

        @pl.when(even)
        def _():
            to_right(left_x, zz, 1).wait_send()

        @pl.when(jnp.logical_not(even))
        def _():
            to_left(right_x, zz, 1).wait_send()

        return carry

    lax.fori_loop(0, NZ, settle_z, 0)

    def other(step):
        h_arrived(slot_of(step, 1 - core))

    other(0)
    h_own.wait_send()

    @pl.when(has_next)
    def _():
        h_next.wait_send()
        h_pass(1).wait_send()
        other(1)

    @pl.when(has_prev)
    def _():
        h_prev.wait_send()
        h_pass(-1).wait_send()
        other(-1)

    @pl.when(has_next & has_prev)
    def _():
        relay_next.wait_send()
        relay_prev.wait_send()

    @pl.when(chip >= 2)
    def _():
        h_pass(-2).wait_send()
        other(-2)

    @pl.when(chip < chips - 2)
    def _():
        h_pass(2).wait_send()
        other(2)

    own_w.wait()
    own_h.wait()


def gather(wide, stem, gain, spread_at, n_tm):
    nx = n_tm // (2 * NZ)
    own = (stem.shape[0], n_tm * wide.shape[0])
    dma = pltpu.SemaphoreType.DMA
    return pl.pallas_call(
        functools.partial(gather_kernel, nx),
        out_shape=(
            jax.ShapeDtypeStruct((n_tm, *wide.shape), wide.dtype),
            jax.ShapeDtypeStruct((4 * REACH + 2, *own), stem.dtype),
        ),
        in_specs=[pl.BlockSpec(memory_space=pltpu.VMEM)] * 4,
        out_specs=(pl.BlockSpec(memory_space=pl.ANY), pl.BlockSpec(memory_space=pl.ANY)),
        scratch_shapes=[
            pltpu.VMEM(own, stem.dtype),
            dma((n_tm,)),
            dma((2, NZ)),
            dma((2, 2 * NZ)),
            dma((n_tm // 2,)),
            dma((4 * REACH + 2,)),
            dma((4,)),
            dma((2 * REACH + 1,)),
            dma((2,)),
        ],
        compiler_params=pltpu.CompilerParams(collective_id=0, has_side_effects=True),
        name="gather",
    )(wide, stem, gain, spread_at)


def deal_kernel(n, out_ref, in_ref, send_sem, recv_sem, own_sem):
    me = lax.axis_index("tm")
    barrier = pltpu.get_barrier_semaphore()

    def peer_of(i):
        return lax.rem(me + i, n)

    def greet(i, carry):
        pl.semaphore_signal(barrier, inc=1, device_id={"tm": peer_of(i)}, device_id_type=MESH)
        return carry

    lax.fori_loop(1, n, greet, 0)
    own = pltpu.make_async_copy(out_ref.at[me], in_ref.at[me], own_sem)
    own.start()
    pl.semaphore_wait(barrier, n - 1)

    def copy(i):
        peer = peer_of(i)
        return pltpu.make_async_remote_copy(
            src_ref=out_ref.at[peer],
            dst_ref=in_ref.at[me],
            send_sem=send_sem.at[i],
            recv_sem=recv_sem.at[me],
            device_id={"tm": peer},
            device_id_type=MESH,
        )

    def send(i, carry):
        copy(i).start()
        return carry

    lax.fori_loop(1, n, send, 0)
    own.wait()

    def settle(i, carry):
        peer = peer_of(i)
        pltpu.make_async_copy(in_ref.at[peer], in_ref.at[peer], recv_sem.at[peer]).wait()
        copy(i).wait_send()
        return carry

    lax.fori_loop(1, n, settle, 0)


def deal(payload):
    n = payload.shape[0]
    dma = pltpu.SemaphoreType.DMA
    return pl.pallas_call(
        functools.partial(deal_kernel, n),
        out_shape=jax.ShapeDtypeStruct(payload.shape, payload.dtype),
        in_specs=[pl.BlockSpec(memory_space=pltpu.VMEM)],
        out_specs=pl.BlockSpec(memory_space=pltpu.VMEM),
        scratch_shapes=[dma((n,)), dma((n,)), dma],
        compiler_params=pltpu.CompilerParams(collective_id=1, has_side_effects=True),
        name="deal",
    )(payload)


def encode_kernel(heads_step, halo_ref, exists_ref, wq_ref, wk_ref, wv_ref, bias_ref, stem_ref, out_ref, clean):
    rows = out_ref.shape[0]

    @pl.when(pl.program_id(0) == 0)
    def _():
        first = lax.rem(lax.axis_index("tm"), 2) * rows
        near = halo_ref[pl.ds(pl.multiple_of(first, rows), clean.shape[0]), :]
        clean[...] = jnp.where(exists_ref[...] > 0, near, jnp.bfloat16(0))

    def project(block, w_ref):
        return jnp.dot(block, w_ref[...], preferred_element_type=jnp.float32).astype(jnp.bfloat16)

    query = project(clean[2 * REACH * rows : (2 * REACH + 1) * rows, :], wq_ref) * jnp.bfloat16(HD ** (-0.5))
    key = project(clean[...], wk_ref)
    value = project(clean[...], wv_ref)
    pair = 2 * HD
    low = lax.broadcasted_iota(jnp.int32, (query.shape[0], pair), 1) < HD
    for p in range(heads_step // 2):
        at = slice(p * pair, (p + 1) * pair)
        parts = []
        for h in range(2):
            mine = low if h == 0 else jnp.logical_not(low)
            scores = lax.dot_general(
                jnp.where(mine, query[:, at], jnp.bfloat16(0)),
                key[:, at],
                (((1,), (1,)), ((), ())),
                preferred_element_type=jnp.float32,
            )
            scores = scores + bias_ref[...]
            raised = jnp.exp(scores - jnp.max(scores, axis=-1, keepdims=True))
            total = jnp.sum(raised, axis=-1, keepdims=True)
            probs = (raised * (1.0 / total)).astype(jnp.bfloat16)
            parts.append(jnp.dot(probs, value[:, at], preferred_element_type=jnp.float32))
        context = jnp.where(low, parts[0], parts[1])
        out_ref[:, at] = (stem_ref[:, at].astype(jnp.float32) + context).astype(jnp.bfloat16)


def encode(halo, exists, weight, bias, stem):
    rows, width = stem.shape
    depth = halo.shape[1]
    around = bias.shape[1]
    heads_step = 4
    span = heads_step * HD
    steps = width // span

    def whole(*shape):
        return pl.BlockSpec(shape, lambda i: (0,) * len(shape))

    def columns(first):
        return pl.BlockSpec((depth, span), lambda i: (0, first * steps + i))

    piece = pl.BlockSpec((rows, span), lambda i: (0, i))
    return pl.pallas_call(
        functools.partial(encode_kernel, heads_step),
        grid=(steps,),
        out_shape=jax.ShapeDtypeStruct(stem.shape, stem.dtype),
        in_specs=[
            whole(*halo.shape),
            whole(around, 1),
            columns(0),
            columns(1),
            columns(2),
            whole(rows, around),
            piece,
        ],
        out_specs=piece,
        scratch_shapes=[pltpu.VMEM((around, depth), jnp.bfloat16)],
        name="encode",
    )(halo, exists, weight, weight, weight, bias, stem)


def layer_norm(block, gain):
    values_in = block.astype(jnp.float32)
    mean = jnp.mean(values_in, axis=-1, keepdims=True)
    var = jnp.mean((values_in - mean) ** 2, axis=-1, keepdims=True)
    return ((values_in - mean) * lax.rsqrt(var + 1e-05) * gain).astype(jnp.bfloat16)


def two_parts(value):
    high = lax.reduce_precision(value, 8, 7)
    return high, lax.reduce_precision(value - high, 8, 7)


def on_device(stem, norm_gain, qkv_weight, segment_ids, dec_queries, stretch_mask):
    rows, width = stem.shape
    heads = width // HD
    scale = HD ** (-0.5)
    tokens_dev = dec_queries.shape[0]
    n_tm = lax.axis_size("tm")
    device = lax.axis_index("tm")
    small = jnp.concatenate(
        [
            dec_queries.reshape(-1),
            stretch_mask.astype(jnp.bfloat16).reshape(-1),
            (segment_ids % 128).astype(jnp.bfloat16),
            (segment_ids // 128).astype(jnp.bfloat16),
        ]
    )
    cuts = [tokens_dev * width, tokens_dev * (width + n_tm)]
    cuts += [cuts[1] + rows, cuts[1] + 2 * rows]
    depth, columns = qkv_weight.shape
    padded = depth + 1 + (-(depth + 1) % 8)
    spread_at = (jnp.arange(width) // depth) * padded + jnp.arange(width) % depth
    small = jnp.pad(small, (0, (padded - depth) * columns - cuts[3])).reshape(-1, columns)
    gathered, halo = gather(
        jnp.concatenate([qkv_weight, small], axis=0),
        stem,
        norm_gain[None, :],
        spread_at[:, None],
        n_tm,
    )
    weight = gathered.reshape(n_tm * padded, columns)
    small_all = gathered[:, depth]
    all_queries = small_all[:, : cuts[0]].reshape(n_tm * tokens_dev, width)
    all_masks = small_all[:, cuts[0] : cuts[1]].reshape(n_tm * tokens_dev, n_tm)
    seg_low = small_all[:, cuts[1] : cuts[2]].reshape(-1).astype(jnp.int32)
    seg_high = small_all[:, cuts[2] : cuts[3]].reshape(-1).astype(jnp.int32)
    around = 4 * REACH + 1
    seg_all = jnp.pad(seg_high * 128 + seg_low, (2 * REACH * rows, 2 * REACH * rows))
    seg_wide = lax.dynamic_slice_in_dim(seg_all, device * rows, around * rows, 0)
    block_at = device - 2 * REACH + jnp.arange(around, dtype=jnp.int32)
    exists = (block_at >= 0) & (block_at < n_tm)
    exists = jnp.repeat(exists.astype(jnp.int32), rows)[:, None]
    same = segment_ids[:, None] == seg_wide[None, :]
    bias = jnp.where(same, jnp.float32(0.0), jnp.float32(-1e30))
    memory = encode(halo.reshape(halo.shape[0] * rows, -1), exists, weight, bias, stem)
    total_tokens = all_queries.shape[0]
    column = lax.dynamic_slice_in_dim(all_masks, device, 1, 1)[:, 0]
    owner = jnp.arange(total_tokens, dtype=jnp.int32) // tokens_dev
    allowed = (column == 1) | (owner == device)
    query_heads = all_queries.reshape(total_tokens, heads, HD)
    memory_heads = memory.reshape(rows, heads, HD)
    cross = (
        jnp.einsum("thd,phd->htp", query_heads, memory_heads, preferred_element_type=jnp.float32)
        * scale
    )
    top_high, top_low = two_parts(jnp.max(cross, axis=-1))
    shift = top_high + top_low
    weights = jnp.where(
        allowed[None, :, None], jnp.exp(cross - shift[:, :, None]), jnp.float32(0.0)
    )
    den_high, den_low = two_parts(jnp.sum(weights, axis=-1))
    numer = jnp.einsum(
        "htp,phd->thd",
        weights.astype(jnp.bfloat16),
        memory_heads,
        preferred_element_type=jnp.float32,
    ).astype(jnp.bfloat16)
    top_high = jnp.where(allowed[None, :], top_high, jnp.float32(-1e30))
    top_low = jnp.where(allowed[None, :], top_low, jnp.float32(0.0))
    stats = jnp.stack([top_high, top_low, den_high, den_low]).astype(jnp.bfloat16)
    stats = jnp.transpose(stats, (2, 0, 1)).reshape(n_tm, -1)
    payload = jnp.concatenate([numer.reshape(n_tm, -1), stats], axis=1)
    payload = jnp.pad(payload, ((0, 0), (0, -payload.shape[1] % 1024)))
    got = deal(payload.reshape(n_tm, -1, 128)).reshape(n_tm, -1).astype(jnp.float32)
    num_all = got[:, : tokens_dev * width].reshape(n_tm, tokens_dev, heads, HD)
    stats = got[:, tokens_dev * width : tokens_dev * (width + 4 * heads)]
    stats = stats.reshape(n_tm, tokens_dev, 4, heads)
    top_all = stats[:, :, 0] + stats[:, :, 1]
    den_all = stats[:, :, 2] + stats[:, :, 3]
    best = jnp.max(top_all, axis=0)
    factor = jnp.exp(top_all - best[None])
    num_total = jnp.sum(factor[..., None] * num_all, axis=0)
    den_total = jnp.sum(factor * den_all, axis=0)
    cross_out = (num_total / den_total[..., None]).reshape(tokens_dev, width).astype(jnp.bfloat16)
    return (memory, cross_out)


def solution(mesh):
    placed = (
        P(("utt", "tm"), None),
        P(),
        P("tm", None),
        P(("utt", "tm")),
        P(("utt", "tm"), None),
        P(("utt", "tm"), None),
    )
    return jax.shard_map(
        on_device,
        mesh=mesh,
        in_specs=placed,
        out_specs=(P(("utt", "tm"), None), P(("utt", "tm"), None)),
        check_vma=False,
    )
```

```python
import functools

import jax
import jax.numpy as jnp
from jax import lax
from jax.experimental import pallas as pl
from jax.experimental.pallas import tpu as pltpu
from jax.sharding import PartitionSpec as P

HD = 64
NZ = 8
REACH = 2
MESH = pl.DeviceIdType.MESH


def gather_kernel(nx, depth, w_ref, stem_ref, gain_ref, wide_ref, halo_ref, own_ref, w_recv, w_zs, w_xs, w_ps, h_recv, h_zs, h_ps, own_sem):
    me = lax.axis_index("tm")
    core = lax.rem(me, 2)
    chip = me // 2
    z = lax.rem(chip, NZ)
    x = chip // NZ
    chips = nx * NZ

    def index(xx, zz):
        return (xx * NZ + zz) * 2 + core

    right_x, left_x, far_x = lax.rem(x + 1, nx), lax.rem(x + nx - 1, nx), lax.rem(x + 2, nx)
    right, left = index(right_x, z), index(left_x, z)
    partner = me + 1 - 2 * core
    up, down = me + 2, me - 2
    has_up, has_down = z < NZ - 1, z > 0
    has_next, has_prev = chip < chips - 1, chip > 0

    barrier = pltpu.get_barrier_semaphore()

    def greet(peer):
        pl.semaphore_signal(barrier, inc=1, device_id={"tm": peer}, device_id_type=MESH)

    greet(right)
    greet(left)
    greet(partner)

    @pl.when(has_next)
    def _():
        greet(up)

    @pl.when(has_prev)
    def _():
        greet(down)

    pl.semaphore_wait(barrier, 3 + has_next.astype(jnp.int32) + has_prev.astype(jnp.int32))

    def w_copy(shard, peer, send_sem, own=False):
        return pltpu.make_async_remote_copy(
            src_ref=w_ref if own else wide_ref.at[shard],
            dst_ref=wide_ref.at[shard],
            send_sem=send_sem,
            recv_sem=w_recv.at[shard],
            device_id={"tm": peer},
            device_id_type=MESH,
        )

    def h_copy(from_slot, to_slot, peer, send_sem, own=False):
        return pltpu.make_async_remote_copy(
            src_ref=own_ref if own else halo_ref.at[from_slot],
            dst_ref=halo_ref.at[to_slot],
            send_sem=send_sem,
            recv_sem=h_recv.at[to_slot],
            device_id={"tm": peer},
            device_id_type=MESH,
        )

    def to_right(xx, zz, slot, own=False):
        return w_copy(index(xx, zz), right, w_xs.at[0, slot * NZ + zz], own)

    def to_left(xx, zz, slot, own=False):
        return w_copy(index(xx, zz), left, w_xs.at[1, slot * NZ + zz], own)

    def to_partner(xx, zz, own=False):
        return w_copy(index(xx, zz), partner, w_ps.at[xx * NZ + zz], own)

    def to_up(zz, own=False):
        return w_copy(index(x, zz), up, w_zs.at[0, zz], own)

    def to_down(zz, own=False):
        return w_copy(index(x, zz), down, w_zs.at[1, zz], own)

    def slot_of(step, cc):
        return (step + REACH) * 2 + cc

    own_slot = slot_of(0, core)
    h_next = h_copy(own_slot, slot_of(-1, core), up, h_zs.at[0], True)
    h_prev = h_copy(own_slot, slot_of(1, core), down, h_zs.at[1], True)
    h_own = h_copy(own_slot, own_slot, partner, h_ps.at[2], True)
    relay_next = h_copy(slot_of(-1, core), slot_of(-2, core), up, h_zs.at[2])
    relay_prev = h_copy(slot_of(1, core), slot_of(2, core), down, h_zs.at[3])

    def h_pass(step):
        slot = slot_of(step, core)
        return h_copy(slot, slot, partner, h_ps.at[step + REACH])

    def w_arrived(shard):
        pltpu.make_async_copy(wide_ref.at[shard], wide_ref.at[shard], w_recv.at[shard]).wait()

    def h_arrived(slot):
        pltpu.make_async_copy(halo_ref.at[slot], halo_ref.at[slot], h_recv.at[slot]).wait()

    @pl.when(has_up)
    def _():
        to_up(z, True).start()

    @pl.when(has_down)
    def _():
        to_down(z, True).start()

    to_right(x, z, 0, True).start()
    to_left(x, z, 0, True).start()
    to_partner(x, z, True).start()
    own_w = pltpu.make_async_copy(w_ref, wide_ref.at[me], own_sem.at[0])
    own_h = pltpu.make_async_copy(own_ref, halo_ref.at[own_slot], own_sem.at[1])
    own_w.start()

    width = stem_ref.shape[1]
    source = lax.broadcasted_iota(jnp.int32, (width, 1), 0)
    shard = lax.shift_right_logical(source * (2**20 // depth + 1), 20)
    lanes = lax.broadcasted_iota(jnp.int32, (width, own_ref.shape[1]), 1)
    spread = jnp.where(lanes == source + shard * (w_ref.shape[0] - depth), 1.0, 0.0).astype(jnp.bfloat16)
    own_ref[...] = jnp.dot(
        layer_norm(stem_ref[...], gain_ref[...]), spread, preferred_element_type=jnp.float32
    ).astype(jnp.bfloat16)

    def beside(zz, fresh):
        ok = (zz >= 0) & (zz < NZ) & fresh

        @pl.when(ok)
        def _():
            even = lax.rem(zz, 2) == 0
            w_arrived(index(left_x, zz))
            to_partner(left_x, zz).start()

            @pl.when(even)
            def _():
                to_right(left_x, zz, 1).start()

            w_arrived(index(right_x, zz))
            to_partner(right_x, zz).start()

            @pl.when(jnp.logical_not(even))
            def _():
                to_left(right_x, zz, 1).start()

    def far(zz, fresh):
        @pl.when((zz >= 0) & (zz < NZ) & fresh)
        def _():
            w_arrived(index(far_x, zz))
            to_partner(far_x, zz).start()

    def step(s, carry):
        below, above = z - s, z + s

        @pl.when((below >= 0) & (s > 0) & (s < NZ))
        def _():
            w_arrived(index(x, below))

            @pl.when(has_up)
            def _():
                to_up(below).start()

            to_right(x, below, 0).start()
            to_left(x, below, 0).start()
            to_partner(x, below).start()

        @pl.when((above < NZ) & (s > 0))
        def _():
            w_arrived(index(x, above))

            @pl.when(has_down)
            def _():
                to_down(above).start()

            to_right(x, above, 0).start()
            to_left(x, above, 0).start()
            to_partner(x, above).start()

        beside(z - (s - 1), s >= 1)
        beside(z + (s - 1), s >= 2)
        far(z - (s - 2), s >= 2)
        far(z + (s - 2), s >= 3)
        return carry

    lax.fori_loop(1, 4, step, 0)

    h_own.start()
    own_h.start()

    @pl.when(has_next)
    def _():
        h_next.start()

    @pl.when(has_prev)
    def _():
        h_prev.start()

    lax.fori_loop(4, NZ, step, 0)

    @pl.when(has_prev)
    def _():
        h_arrived(slot_of(-1, core))
        h_pass(-1).start()

        @pl.when(has_next)
        def _():
            relay_next.start()

    @pl.when(has_next)
    def _():
        h_arrived(slot_of(1, core))
        h_pass(1).start()

        @pl.when(has_prev)
        def _():
            relay_prev.start()

    lax.fori_loop(NZ, NZ + 2, step, 0)

    @pl.when(chip >= 2)
    def _():
        h_arrived(slot_of(-2, core))
        h_pass(-2).start()

    @pl.when(chip < chips - 2)
    def _():
        h_arrived(slot_of(2, core))
        h_pass(2).start()

    def settle(i, carry):
        w_arrived(i * 2 + 1 - core)
        to_partner(i // NZ, lax.rem(i, NZ), False).wait_send()
        return carry

    lax.fori_loop(0, chips, settle, 0)

    def settle_z(zz, carry):
        @pl.when((zz <= z) & has_up)
        def _():
            to_up(zz).wait_send()

        @pl.when((zz >= z) & has_down)
        def _():
            to_down(zz).wait_send()

        to_right(x, zz, 0).wait_send()
        to_left(x, zz, 0).wait_send()
        even = lax.rem(zz, 2) == 0

        @pl.when(even)
        def _():
            to_right(left_x, zz, 1).wait_send()

        @pl.when(jnp.logical_not(even))
        def _():
            to_left(right_x, zz, 1).wait_send()

        return carry

    lax.fori_loop(0, NZ, settle_z, 0)

    def other(step):
        h_arrived(slot_of(step, 1 - core))

    other(0)
    h_own.wait_send()

    @pl.when(has_next)
    def _():
        h_next.wait_send()
        h_pass(1).wait_send()
        other(1)

    @pl.when(has_prev)
    def _():
        h_prev.wait_send()
        h_pass(-1).wait_send()
        other(-1)

    @pl.when(has_next & has_prev)
    def _():
        relay_next.wait_send()
        relay_prev.wait_send()

    @pl.when(chip >= 2)
    def _():
        h_pass(-2).wait_send()
        other(-2)

    @pl.when(chip < chips - 2)
    def _():
        h_pass(2).wait_send()
        other(2)

    own_w.wait()
    own_h.wait()


def gather(wide, depth, stem, gain, n_tm):
    nx = n_tm // (2 * NZ)
    own = (stem.shape[0], n_tm * wide.shape[0])
    dma = pltpu.SemaphoreType.DMA
    return pl.pallas_call(
        functools.partial(gather_kernel, nx, depth),
        out_shape=(
            jax.ShapeDtypeStruct((n_tm, *wide.shape), wide.dtype),
            jax.ShapeDtypeStruct((4 * REACH + 2, *own), stem.dtype),
        ),
        in_specs=[pl.BlockSpec(memory_space=pltpu.VMEM)] * 3,
        out_specs=(pl.BlockSpec(memory_space=pl.ANY), pl.BlockSpec(memory_space=pl.ANY)),
        scratch_shapes=[
            pltpu.VMEM(own, stem.dtype),
            dma((n_tm,)),
            dma((2, NZ)),
            dma((2, 2 * NZ)),
            dma((n_tm // 2,)),
            dma((4 * REACH + 2,)),
            dma((4,)),
            dma((2 * REACH + 1,)),
            dma((2,)),
        ],
        compiler_params=pltpu.CompilerParams(collective_id=0, has_side_effects=True),
        name="gather",
    )(wide, stem, gain)


def deal_kernel(n, out_ref, in_ref, send_sem, recv_sem, own_sem):
    me = lax.axis_index("tm")
    barrier = pltpu.get_barrier_semaphore()

    def peer_of(i):
        return lax.rem(me + i, n)

    def greet(i, carry):
        pl.semaphore_signal(barrier, inc=1, device_id={"tm": peer_of(i)}, device_id_type=MESH)
        return carry

    lax.fori_loop(1, n, greet, 0)
    own = pltpu.make_async_copy(out_ref.at[me], in_ref.at[me], own_sem)
    own.start()
    pl.semaphore_wait(barrier, n - 1)

    def copy(i):
        peer = peer_of(i)
        return pltpu.make_async_remote_copy(
            src_ref=out_ref.at[peer],
            dst_ref=in_ref.at[me],
            send_sem=send_sem.at[i],
            recv_sem=recv_sem.at[me],
            device_id={"tm": peer},
            device_id_type=MESH,
        )

    def send(i, carry):
        copy(i).start()
        return carry

    lax.fori_loop(1, n, send, 0)
    own.wait()

    def settle(i, carry):
        peer = peer_of(i)
        pltpu.make_async_copy(in_ref.at[peer], in_ref.at[peer], recv_sem.at[peer]).wait()
        copy(i).wait_send()
        return carry

    lax.fori_loop(1, n, settle, 0)


def deal(payload):
    n = payload.shape[0]
    dma = pltpu.SemaphoreType.DMA
    return pl.pallas_call(
        functools.partial(deal_kernel, n),
        out_shape=jax.ShapeDtypeStruct(payload.shape, payload.dtype),
        in_specs=[pl.BlockSpec(memory_space=pltpu.VMEM)],
        out_specs=pl.BlockSpec(memory_space=pltpu.VMEM),
        scratch_shapes=[dma((n,)), dma((n,)), dma],
        compiler_params=pltpu.CompilerParams(collective_id=1, has_side_effects=True),
        name="deal",
    )(payload)


def encode_kernel(heads_step, halo_ref, wq_ref, wk_ref, wv_ref, bias_ref, stem_ref, out_ref, clean):
    rows = out_ref.shape[0]

    @pl.when(pl.program_id(0) == 0)
    def _():
        me = lax.axis_index("tm")
        first = lax.rem(me, 2) * rows
        near = halo_ref[pl.ds(pl.multiple_of(first, rows), clean.shape[0]), :]
        place = lax.broadcasted_iota(jnp.int32, near.shape, 0) + (me - 2 * REACH) * rows
        exists = (place >= 0) & (place < lax.axis_size("tm") * rows)
        clean[...] = jnp.where(exists, near, jnp.bfloat16(0))

    def project(block, w_ref):
        return jnp.dot(block, w_ref[...], preferred_element_type=jnp.float32).astype(jnp.bfloat16)

    query = project(clean[2 * REACH * rows : (2 * REACH + 1) * rows, :], wq_ref) * jnp.bfloat16(HD ** (-0.5))
    key = project(clean[...], wk_ref)
    value = project(clean[...], wv_ref)
    pair = 2 * HD
    low = lax.broadcasted_iota(jnp.int32, (query.shape[0], pair), 1) < HD
    for p in range(heads_step // 2):
        at = slice(p * pair, (p + 1) * pair)
        parts = []
        for h in range(2):
            mine = low if h == 0 else jnp.logical_not(low)
            scores = lax.dot_general(
                jnp.where(mine, query[:, at], jnp.bfloat16(0)),
                key[:, at],
                (((1,), (1,)), ((), ())),
                preferred_element_type=jnp.float32,
            )
            scores = scores + bias_ref[...]
            raised = jnp.exp(scores - jnp.max(scores, axis=-1, keepdims=True))
            total = jnp.sum(raised, axis=-1, keepdims=True)
            probs = (raised * (1.0 / total)).astype(jnp.bfloat16)
            parts.append(jnp.dot(probs, value[:, at], preferred_element_type=jnp.float32))
        context = jnp.where(low, parts[0], parts[1])
        out_ref[:, at] = (stem_ref[:, at].astype(jnp.float32) + context).astype(jnp.bfloat16)


def encode(halo, weight, bias, stem):
    rows, width = stem.shape
    depth = halo.shape[1]
    around = bias.shape[1]
    heads_step = 4
    span = heads_step * HD
    steps = width // span

    def whole(*shape):
        return pl.BlockSpec(shape, lambda i: (0,) * len(shape))

    def columns(first):
        return pl.BlockSpec((depth, span), lambda i: (0, first * steps + i))

    piece = pl.BlockSpec((rows, span), lambda i: (0, i))
    return pl.pallas_call(
        functools.partial(encode_kernel, heads_step),
        grid=(steps,),
        out_shape=jax.ShapeDtypeStruct(stem.shape, stem.dtype),
        in_specs=[
            whole(*halo.shape),
            columns(0),
            columns(1),
            columns(2),
            whole(rows, around),
            piece,
        ],
        out_specs=piece,
        scratch_shapes=[pltpu.VMEM((around, depth), jnp.bfloat16)],
        name="encode",
    )(halo, weight, weight, weight, bias, stem)


def layer_norm(block, gain):
    values_in = block.astype(jnp.float32)
    mean = jnp.mean(values_in, axis=-1, keepdims=True)
    var = jnp.mean((values_in - mean) ** 2, axis=-1, keepdims=True)
    return ((values_in - mean) * lax.rsqrt(var + 1e-05) * gain).astype(jnp.bfloat16)


def two_parts(value):
    high = lax.reduce_precision(value, 8, 7)
    return high, lax.reduce_precision(value - high, 8, 7)


def on_device(stem, norm_gain, qkv_weight, segment_ids, dec_queries, stretch_mask):
    rows, width = stem.shape
    heads = width // HD
    scale = HD ** (-0.5)
    tokens_dev = dec_queries.shape[0]
    n_tm = lax.axis_size("tm")
    device = lax.axis_index("tm")
    small = jnp.concatenate(
        [
            dec_queries.reshape(-1),
            stretch_mask.astype(jnp.bfloat16).reshape(-1),
            (segment_ids % 128).astype(jnp.bfloat16),
            (segment_ids // 128).astype(jnp.bfloat16),
        ]
    )
    cuts = [tokens_dev * width, tokens_dev * (width + n_tm)]
    cuts += [cuts[1] + rows, cuts[1] + 2 * rows]
    depth, columns = qkv_weight.shape
    padded = depth + 1 + (-(depth + 1) % 8)
    small = jnp.pad(small, (0, (padded - depth) * columns - cuts[3])).reshape(-1, columns)
    gathered, halo = gather(
        jnp.concatenate([qkv_weight, small], axis=0),
        depth,
        stem,
        norm_gain[None, :],
        n_tm,
    )
    weight = gathered.reshape(n_tm * padded, columns)
    small_all = gathered[:, depth]
    all_queries = small_all[:, : cuts[0]].reshape(n_tm * tokens_dev, width)
    all_masks = small_all[:, cuts[0] : cuts[1]].reshape(n_tm * tokens_dev, n_tm)
    seg_low = small_all[:, cuts[1] : cuts[2]].reshape(-1).astype(jnp.int32)
    seg_high = small_all[:, cuts[2] : cuts[3]].reshape(-1).astype(jnp.int32)
    around = 4 * REACH + 1
    seg_all = jnp.pad(seg_high * 128 + seg_low, (2 * REACH * rows, 2 * REACH * rows))
    seg_wide = lax.dynamic_slice_in_dim(seg_all, device * rows, around * rows, 0)
    same = segment_ids[:, None] == seg_wide[None, :]
    bias = jnp.where(same, jnp.float32(0.0), jnp.float32(-1e30))
    memory = encode(halo.reshape(halo.shape[0] * rows, -1), weight, bias, stem)
    total_tokens = all_queries.shape[0]
    column = lax.dynamic_slice_in_dim(all_masks, device, 1, 1)[:, 0]
    owner = jnp.arange(total_tokens, dtype=jnp.int32) // tokens_dev
    allowed = (column == 1) | (owner == device)
    query_heads = all_queries.reshape(total_tokens, heads, HD)
    memory_heads = memory.reshape(rows, heads, HD)
    cross = (
        jnp.einsum("thd,phd->htp", query_heads, memory_heads, preferred_element_type=jnp.float32)
        * scale
    )
    top_high, top_low = two_parts(jnp.max(cross, axis=-1))
    shift = top_high + top_low
    weights = jnp.where(
        allowed[None, :, None], jnp.exp(cross - shift[:, :, None]), jnp.float32(0.0)
    )
    den_high, den_low = two_parts(jnp.sum(weights, axis=-1))
    numer = jnp.einsum(
        "htp,phd->thd",
        weights.astype(jnp.bfloat16),
        memory_heads,
        preferred_element_type=jnp.float32,
    ).astype(jnp.bfloat16)
    top_high = jnp.where(allowed[None, :], top_high, jnp.float32(-1e30))
    top_low = jnp.where(allowed[None, :], top_low, jnp.float32(0.0))
    stats = jnp.stack([top_high, top_low, den_high, den_low]).astype(jnp.bfloat16)
    stats = jnp.transpose(stats, (2, 0, 1)).reshape(n_tm, -1)
    payload = jnp.concatenate([numer.reshape(n_tm, -1), stats], axis=1)
    payload = jnp.pad(payload, ((0, 0), (0, -payload.shape[1] % 1024)))
    got = deal(payload.reshape(n_tm, -1, 128)).reshape(n_tm, -1).astype(jnp.float32)
    num_all = got[:, : tokens_dev * width].reshape(n_tm, tokens_dev, heads, HD)
    stats = got[:, tokens_dev * width : tokens_dev * (width + 4 * heads)]
    stats = stats.reshape(n_tm, tokens_dev, 4, heads)
    top_all = stats[:, :, 0] + stats[:, :, 1]
    den_all = stats[:, :, 2] + stats[:, :, 3]
    best = jnp.max(top_all, axis=0)
    factor = jnp.exp(top_all - best[None])
    num_total = jnp.sum(factor[..., None] * num_all, axis=0)
    den_total = jnp.sum(factor * den_all, axis=0)
    cross_out = (num_total / den_total[..., None]).reshape(tokens_dev, width).astype(jnp.bfloat16)
    return (memory, cross_out)


def solution(mesh):
    placed = (
        P(("utt", "tm"), None),
        P(),
        P("tm", None),
        P(("utt", "tm")),
        P(("utt", "tm"), None),
        P(("utt", "tm"), None),
    )
    return jax.shard_map(
        on_device,
        mesh=mesh,
        in_specs=placed,
        out_specs=(P(("utt", "tm"), None), P(("utt", "tm"), None)),
        check_vma=False,
    )
```
